32 devices in a mesh: sfc: 16 (over z, x, core), lvl: 2 (over y).
Axes of the slice: x: 2, y: 2, z: 4, core: 2. Of those that a mesh axis runs over, the one named last changes fastest.
Arguments:
- right_side: float32 [16384, 128], P(('sfc', 'lvl')), may hold values from -48 to 48
- cell_coef: float32 [16384], P(('sfc', 'lvl')), may hold values from 4 to 16
- fine_count: int32 [32], replicated, may hold values from 256 to 512, as said below
- cell_matrix: float32 [128, 128], replicated, may hold values from -0.5 to 0.5
- face_near: float32 [128, 128], replicated, may hold values from -0.5 to 0.5
- face_far: float32 [128, 128], replicated, may hold values from -0.5 to 0.5
- prolong: float32 [8, 128, 128], replicated, may hold values from -0.5 to 0.5
Outputs:
- solution: float32 [16384, 128], P(('sfc', 'lvl'))
The draws below stay inside these ranges and needn't reach their ends.
Inputs may be any that keep to these rules, and one draw needn't show every extreme that they name: `fine_count`: each device's count is a multiple of 8 and at least 256; exactly one device holds 512, every other at most 504.
All inputs are finite; a program needn't handle non-finite values.
Results may differ from the reference program's by a relative error of at most 0.000051.
Values sent between devices are 32-bit elements; how exact they have to be, the bound alone decides.
No kernel may reach another device: no remote copies, remote signals or barrier semaphores. Data moves between devices by JAX's collectives and lax.ppermute only.
A program may use at most 64 MiB of HBM per device.

```python
import math
import jax
import jax.numpy as jnp
from jax import lax

V = 128
CAP = 512
DEG = 3
W = 32
WC = 32
SLOTS = 16384
DEVICES = 32


def draw_fine_count(key, part):
    key_values, key_top = jax.random.split(jax.random.fold_in(key, 17))
    counts = jax.random.randint(key_values, (DEVICES,), CAP // 16, CAP // 8) * 8
    fullest = jax.random.randint(key_top, (), 0, DEVICES)
    return counts.at[fullest].set(CAP).astype(jnp.int32)


def shard_levels(own_key, dims, pieces, low, high):
    gain = 1.0
    for axis_at, shards_of in pieces:
        steps = jax.random.uniform(jax.random.fold_in(jax.random.fold_in(own_key, 6), axis_at), (shards_of,), jnp.float32, low / len(pieces), high / len(pieces))
        gain = gain * jnp.repeat(jnp.exp(steps), dims[axis_at] // shards_of).reshape((-1,) + (1,) * (len(dims) - 1 - axis_at))
    return gain


def gaussian(own_key, extent, spread, limit, shards=(), held_as=jnp.bfloat16):
    values = jax.random.normal(own_key, extent, jnp.float32) * spread
    if len(shards) > 0:
        values = shard_levels(own_key, extent, shards, -0.22, 0.18) * values
    return jnp.clip(values, min=-limit, max=limit).astype(held_as)


def setup_inputs(seed: int = 0) -> dict:
    arg_keys = jax.random.split(jax.random.key(seed), 8)
    right_side = gaussian(arg_keys[0], (SLOTS, V), 8.0, 48.0, ((0, 32),), jnp.float32)
    cell_coef = jnp.clip(jnp.exp(math.log(16.0) - 1.3862944 * jax.random.uniform(arg_keys[1], (SLOTS,), jnp.float32) ** shard_levels(arg_keys[1], (SLOTS,), ((0, 32),), -0.2, 0.2)), 4.0, 16.0)
    fine_count = draw_fine_count(jax.random.fold_in(arg_keys[7], 71), 0)
    cell_matrix = gaussian(arg_keys[3], (V, V), V ** -0.5, 0.5, (), jnp.float32)
    face_near = gaussian(arg_keys[4], (V, V), V ** -0.5, 0.5, (), jnp.float32)
    face_far = gaussian(arg_keys[5], (V, V), V ** -0.5, 0.5, (), jnp.float32)
    prolong = gaussian(arg_keys[6], (8, V, V), V ** -0.5, 0.5, (), jnp.float32)
    return {"right_side": right_side, "cell_coef": cell_coef, "fine_count": fine_count, "cell_matrix": cell_matrix, "face_near": face_near, "face_far": face_far, "prolong": prolong}


def shifted_dot(field, matrix):
    return jnp.dot(field, matrix, precision=lax.Precision.HIGHEST, preferred_element_type=jnp.float32)


def chain_apply(field, chain_coef, is_live, stride, cell_matrix, face_near, face_far):
    zero_one = jnp.zeros((1, field.shape[1]), jnp.float32)
    zero_far = jnp.zeros((stride, field.shape[1]), jnp.float32)
    next_one = jnp.concatenate([field[1:], zero_one], 0)
    prev_one = jnp.concatenate([zero_one, field[:-1]], 0)
    next_far = jnp.concatenate([field[stride:], zero_far], 0)
    prev_far = jnp.concatenate([zero_far, field[:-stride]], 0)
    result = chain_coef[:, None] * field + shifted_dot(field, cell_matrix)
    result = result - shifted_dot(next_one, face_near) - shifted_dot(prev_one, face_near.T)
    result = result - shifted_dot(next_far, face_far) - shifted_dot(prev_far, face_far.T)
    return jnp.where(is_live[:, None], result, 0.0)


def jacobi_scale(chain_coef, is_live, cell_diag):
    safe_coef = jnp.where(is_live, chain_coef, 16.0)
    return jnp.where(is_live[:, None], 1.0 / (safe_coef[:, None] + cell_diag[None, :]), 0.0)


def chebyshev(apply_fn, jacobi, source, start):
    center = 1.025
    radius = 0.775
    sigma_ratio = center / radius
    if start is None:
        residual = source
    else:
        residual = source - apply_fn(start)
    update = jacobi * residual / center
    iterate = update if start is None else start + update
    weight_prev = 1.0 / sigma_ratio
    for repeat in range(DEG - 1):
        weight_next = 1.0 / (2.0 * sigma_ratio - weight_prev)
        residual = source - apply_fn(iterate)
        update = weight_next * weight_prev * update + (2.0 * weight_next / radius) * jacobi * residual
        iterate = iterate + update
        weight_prev = weight_next
    return iterate


def reference(right_side, cell_coef, fine_count, cell_matrix, face_near, face_far, prolong):
    total_slots = right_side.shape[0]
    values = right_side.shape[1]
    slot_index = jnp.arange(total_slots, dtype=jnp.int32)
    owner = (slot_index // CAP).astype(jnp.int32)
    is_slot_live = (slot_index % CAP) < fine_count[owner]
    chain_rank = (jnp.cumsum(is_slot_live.astype(jnp.int32)) - 1).astype(jnp.int32)
    chain_slot = jnp.where(is_slot_live, chain_rank, total_slots).astype(jnp.int32)
    live_total = jnp.sum(fine_count)
    source = jnp.zeros_like(right_side).at[chain_slot].set(right_side, mode="drop")
    chain_coef = jnp.zeros_like(cell_coef).at[chain_slot].set(cell_coef, mode="drop")
    is_live = slot_index < live_total
    cell_diag = jnp.diagonal(cell_matrix)
    jacobi = jacobi_scale(chain_coef, is_live, cell_diag)

    def fine_apply(field):
        return chain_apply(field, chain_coef, is_live, W, cell_matrix, face_near, face_far)

    iterate = chebyshev(fine_apply, jacobi, source, None)
    residual = source - fine_apply(iterate)
    restrict_map = jnp.transpose(prolong, (0, 2, 1)).reshape(8 * values, values)
    coarse_source = jnp.dot(residual.reshape(total_slots // 8, 8 * values), restrict_map, precision=lax.Precision.HIGHEST, preferred_element_type=jnp.float32)
    coarse_coef = jnp.mean(chain_coef.reshape(total_slots // 8, 8), axis=1)
    coarse_index = jnp.arange(total_slots // 8, dtype=jnp.int32)
    is_coarse = coarse_index < live_total // 8
    coarse_jacobi = jacobi_scale(coarse_coef, is_coarse, cell_diag)

    def coarse_apply(field):
        return chain_apply(field, coarse_coef, is_coarse, WC, cell_matrix, face_near, face_far)

    correction = chebyshev(coarse_apply, coarse_jacobi, coarse_source, None)
    prolong_map = jnp.transpose(prolong, (1, 0, 2)).reshape(values, 8 * values)
    iterate = iterate + jnp.dot(correction, prolong_map, precision=lax.Precision.HIGHEST, preferred_element_type=jnp.float32).reshape(total_slots, values)
    iterate = chebyshev(fine_apply, jacobi, source, iterate)
    gathered = iterate[jnp.maximum(chain_rank, 0)]
    return jnp.where(is_slot_live[:, None], gathered, 0.0)
```

```python
import jax
import jax.numpy as jnp
from jax import lax
from jax.experimental import pallas as pl
from jax.experimental.pallas import tpu as pltpu
from jax.sharding import PartitionSpec as P

DEG = 3
AXES = ("sfc", "lvl")
CENTER = 1.025
RADIUS = 0.775
CHILDREN = 8


def chebyshev_weights():
    sigma = CENTER / RADIUS
    weight = 1.0 / sigma
    steps = [(0.0, 1.0 / CENTER)]
    for _ in range(DEG - 1):
        following = 1.0 / (2.0 * sigma - weight)
        steps.append((following * weight, 2.0 * following / RADIUS))
        weight = following
    return steps


STEPS = chebyshev_weights()


def step_weights(step):
    keep = jnp.float32(STEPS[0][0])
    gain = jnp.float32(STEPS[0][1])
    for index in range(1, DEG):
        keep = jnp.where(step == index, jnp.float32(STEPS[index][0]), keep)
        gain = jnp.where(step == index, jnp.float32(STEPS[index][1]), gain)
    return keep, gain


def device_number():
    return lax.axis_index("sfc") * lax.axis_size("lvl") + lax.axis_index("lvl")


def device_total():
    return lax.axis_size("sfc") * lax.axis_size("lvl")


def halves(value):
    high = value.astype(jnp.bfloat16)
    low = (value - high.astype(jnp.float32)).astype(jnp.bfloat16)
    return high, low


def dot(left, right):
    return jnp.dot(left, right, preferred_element_type=jnp.float32)


def product(parts, pair):
    width = pair.shape[1] // 2
    split = [halves(part) for part in parts]
    high = jnp.concatenate([one[0] for one in split], 1)
    low = jnp.concatenate([one[1] for one in split], 1)
    both = dot(high, pair[...])
    return both[:, :width] + both[:, width:] + dot(low, pair[:, :width])


def neighbours(field, start, rows, stride):
    return [field[pl.ds(start + shift, rows), :] for shift in (0, 1, -1, stride, -stride)]


def columns(row, lanes):
    return jnp.transpose(jnp.broadcast_to(row, (lanes, lanes)))


def pack_kernel(count, right_side, coef, first, second, turned):
    values = right_side.shape[1]
    depth = first.shape[0] - 8
    device = device_number()
    live = count[device]
    is_even = device % 2 == 0
    tail = pl.multiple_of(live - depth, 8)
    for out, start in (
        (first, jnp.where(is_even, tail, 0)),
        (second, jnp.where(is_even, 0, tail)),
    ):
        start = pl.multiple_of(start, 8)
        out[:depth, :] = right_side[pl.ds(start, depth), :]
        row = start // values
        lane = start % values
        turned[: coef.shape[0], :] = pltpu.roll(coef[...], (values - lane) % values, 1)
        lanes = lax.broadcasted_iota(jnp.int32, (8, values), 1)
        near = turned[pl.ds(row, 8), :]
        far = turned[pl.ds(row + 1, 8), :]
        out[depth:, :] = jnp.where(lanes < values - lane, near, far)


def prepare_kernel(
    cell_matrix, face_near, face_far, prolong, coef, coupling, restrict, spread, own_coef, own_jacobi, diag
):
    values = cell_matrix.shape[0]
    near = face_near[...]
    far = face_far[...]
    blocks = (cell_matrix[...], -near, -jnp.transpose(near), -far, -jnp.transpose(far))
    for index, block in enumerate(blocks):
        rows = pl.ds(index * values, values)
        high, low = halves(block)
        coupling[rows, :values] = high
        coupling[rows, values:] = low
    for child in range(CHILDREN):
        rows = pl.ds(child * values, values)
        block = prolong[child]
        high, low = halves(block)
        spread[:values, rows] = high
        spread[values:, rows] = low
        high, low = halves(jnp.transpose(block))
        restrict[rows, :values] = high
        restrict[rows, values:] = low
    row_index = lax.broadcasted_iota(jnp.int32, (values, values), 0)
    lane_index = lax.broadcasted_iota(jnp.int32, (values, values), 1)
    diagonal = jnp.sum(
        jnp.where(row_index == lane_index, cell_matrix[...], 0.0), axis=0, keepdims=True
    )
    diag[...] = jnp.broadcast_to(diagonal, diag.shape)
    for row in range(coef.shape[0]):
        rows = pl.ds(row * values, values)
        column = columns(coef[row : row + 1, :], values)
        own_coef[rows, :] = column
        own_jacobi[rows, :] = 1.0 / (column + diagonal)


def fine_kernel(
    count, right_side, first, second, coupling, restrict, own_coef, own_jacobi, diag,
    iterate, residual, coef, jacobi, message, update, coarse_coef,
):
    capacity, values = right_side.shape
    stride = capacity // 16
    depth = first.shape[0] - 8
    frame = capacity + 2 * depth
    device = device_number()
    total = device_total()
    live = count[device]
    is_even = device % 2 == 0
    end = pl.multiple_of(depth + live, 8)
    left = jnp.where(is_even, second[...], first[...])
    right = jnp.where(is_even, first[...], second[...])
    diagonal = diag[0:1, :]

    def column_of(side):
        pieces = []
        for row in range(-(-depth // values)):
            pieces.append(columns(side[depth + row : depth + row + 1, :], values))
        return jnp.concatenate(pieces, 0)[:depth]

    left_coef = column_of(left)
    right_coef = column_of(right)
    residual[:depth, :] = left[:depth]
    residual[pl.ds(depth, capacity), :] = right_side[...]
    residual[pl.ds(depth + capacity, depth), :] = jnp.zeros((depth, values), jnp.float32)
    residual[pl.ds(end, depth), :] = right[:depth]
    coef[:depth, :] = left_coef
    coef[pl.ds(depth, capacity), :] = own_coef[...]
    coef[pl.ds(depth + capacity, depth), :] = jnp.zeros((depth, values), jnp.float32)
    coef[pl.ds(end, depth), :] = right_coef
    jacobi[:depth, :] = jnp.where(device > 0, 1.0 / (left_coef + diagonal), 0.0)
    jacobi[pl.ds(depth, capacity), :] = own_jacobi[...]
    jacobi[pl.ds(depth + capacity, depth), :] = jnp.zeros((depth, values), jnp.float32)
    jacobi[pl.ds(end, depth), :] = jnp.where(device < total - 1, 1.0 / (right_coef + diagonal), 0.0)
    update[...] = jnp.zeros(update.shape, jnp.float32)
    iterate[...] = jnp.zeros(iterate.shape, jnp.float32)

    def step(index, carry):
        keep, gain = step_weights(index)
        fresh = keep * update[...] + gain * (jacobi[...] * residual[...])
        update[...] = fresh
        iterate[...] += fresh
        span = (frame - 2 * stride) // 2
        for block in range(2):
            start = stride + block * span
            rows = pl.ds(start, span)
            applied = product(neighbours(update, start, span, stride), coupling)
            residual[rows, :] = residual[rows, :] - (coef[rows, :] * update[rows, :] + applied)
        return carry

    lax.fori_loop(0, DEG, step, 0)
    cells = message.shape[0] - 8
    first_row = depth - CHILDREN * ((cells - capacity // CHILDREN) // 2)
    parts = [residual[pl.ds(first_row + c, cells, stride=CHILDREN), :] for c in range(CHILDREN)]
    message[:cells, :] = product(parts, restrict)
    mean = coef[pl.ds(first_row, cells, stride=CHILDREN), :]
    for c in range(1, CHILDREN):
        mean = mean + coef[pl.ds(first_row + c, cells, stride=CHILDREN), :]
    coarse_coef[...] = jnp.zeros(coarse_coef.shape, jnp.float32)
    coarse_coef[:cells, :] = mean * (1.0 / CHILDREN)
    message[cells:, :] = jnp.transpose(coarse_coef[...])[:8]


def coarse_kernel(
    count, iterate, residual, coef, jacobi, own, before_one, before_two, after_one, after_two,
    coupling, spread, diag, out, solved, source, coarse_coef, coarse_jacobi, coarse_update, coarse, update,
):
    capacity, values = out.shape
    stride = capacity // 16
    slots = capacity // CHILDREN
    margin = (own.shape[0] - 8 - slots) // 2
    depth = (iterate.shape[0] - capacity) // 2
    reach = depth // 2 // CHILDREN
    base = 2 * slots + margin
    device = device_number()
    total = device_total()

    def cells_of(offset):
        at = device + offset
        inside = (at >= 0) & (at < total)
        return jnp.where(inside, count[jnp.clip(at, 0, total - 1)] // CHILDREN, 0)

    size = cells_of(0)
    start_before = base - cells_of(-1)
    start_after = base + size
    start_last = start_after + cells_of(1)
    source[...] = jnp.zeros(source.shape, jnp.float32)
    coarse_coef[...] = jnp.zeros(coarse_coef.shape, jnp.float32)
    placed = (
        (before_two, start_before - cells_of(-2) - margin, 0, slots + 2 * margin),
        (before_one, start_before, margin, slots),
        (own, base, margin, slots),
        (after_one, start_after, margin, slots),
        (after_two, start_last, margin, slots + margin),
    )
    for piece, at, begin, rows in placed:
        source[pl.ds(at, rows), :] = piece[begin : begin + rows, :]
        column = columns(piece[slots + 2 * margin : slots + 2 * margin + 1, :], values)
        coarse_coef[pl.ds(at, rows), :] = column[begin : begin + rows]
    lowest = start_before - cells_of(-2) - jnp.where(device > 2, margin, 0)
    highest = start_last + cells_of(2) + jnp.where(device < total - 3, margin, 0)
    row_index = lax.broadcasted_iota(jnp.int32, source.shape, 0)
    inside = (row_index >= lowest) & (row_index < highest)
    coarse_jacobi[...] = jnp.where(inside, 1.0 / (coarse_coef[...] + diag[0:1, :]), 0.0)
    fresh = STEPS[0][1] * (coarse_jacobi[...] * source[...])
    coarse_update[...] = fresh
    coarse[...] = fresh
    low = base - slots - margin
    high = base + 2 * slots + margin
    for index in range(1, DEG):
        keep, gain = STEPS[index]
        rows = pl.ds(low, high - low)
        applied = product(neighbours(coarse_update, low, high - low, stride), coupling)
        source[rows, :] = source[rows, :] - (coarse_coef[rows, :] * coarse_update[rows, :] + applied)
        fresh = keep * coarse_update[rows, :] + gain * (coarse_jacobi[rows, :] * source[rows, :])
        coarse_update[rows, :] = fresh
        coarse[rows, :] += fresh
    count_rows = slots + 2 * reach
    correction = coarse[pl.ds(base - reach, count_rows), :]
    high_part, low_part = halves(correction)
    spread_high = spread[:values, :]
    children = dot(high_part, spread_high) + dot(low_part, spread_high) + dot(high_part, spread[values:, :])
    first_row = depth - CHILDREN * reach
    for c in range(CHILDREN):
        update[pl.ds(first_row + c, count_rows, stride=CHILDREN), :] = children[:, c * values : (c + 1) * values]
    used = pl.ds(first_row, CHILDREN * count_rows)
    solved[used, :] = iterate[used, :] + update[used, :]
    work = pl.ds(first_row, CHILDREN * count_rows)
    update[pl.ds(first_row - stride, stride), :] = jnp.zeros((stride, values), jnp.float32)
    update[pl.ds(first_row + CHILDREN * count_rows, stride), :] = jnp.zeros((stride, values), jnp.float32)
    solved_residual = residual

    def step(index, carry):
        keep, gain = step_weights(index)
        span = (CHILDREN * count_rows - 2 * stride) // 2
        for block in range(2):
            start = first_row + stride + block * span
            rows = pl.ds(start, span)
            applied = product(neighbours(update, start, span, stride), coupling)
            solved_residual[rows, :] = solved_residual[rows, :] - (coef[rows, :] * update[rows, :] + applied)
        fresh = keep * update[work, :] + gain * (jacobi[work, :] * solved_residual[work, :])
        update[work, :] = fresh
        solved[work, :] += fresh
        return carry

    lax.fori_loop(0, DEG, step, 0)
    live = count[device]
    is_live = lax.broadcasted_iota(jnp.int32, (capacity, values), 0) < live
    out[...] = jnp.where(is_live, solved[pl.ds(depth, capacity), :], 0.0)


def exchange(block, distance, phase):
    total = lax.axis_size(AXES)
    pairs = []
    for device in range(total - distance):
        if (device // distance) % 2 == phase:
            pairs += [(device, device + distance), (device + distance, device)]
    return lax.ppermute(block, AXES, pairs)


def shards(right_side, cell_coef, fine_count, cell_matrix, face_near, face_far, prolong):
    capacity, values = right_side.shape
    stride = capacity // 16
    depth = 6 * stride
    frame = capacity + 2 * depth
    slots = capacity // CHILDREN
    margin = 16
    coef_rows = jnp.concatenate(
        [cell_coef.reshape(capacity // values, values), jnp.ones((8 - capacity // values, values), jnp.float32)], 0
    )
    f32 = lambda *shape: jax.ShapeDtypeStruct(shape, jnp.float32)
    bf16 = lambda *shape: jax.ShapeDtypeStruct(shape, jnp.bfloat16)
    buffer = lambda *shape: pltpu.VMEM(shape, jnp.float32)
    smem = pl.BlockSpec(memory_space=pltpu.SMEM)
    vmem = pl.BlockSpec(memory_space=pltpu.VMEM)

    first, second = pl.pallas_call(
        pack_kernel,
        out_shape=(f32(depth + 8, values), f32(depth + 8, values)),
        in_specs=[smem, vmem, vmem],
        out_specs=(vmem, vmem),
        scratch_shapes=[buffer(24, values)],
        name="pack",
    )(fine_count, right_side, coef_rows)
    first_in = exchange(first, 1, 0)
    second_in = exchange(second, 1, 1)
    coupling, restrict, spread, own_coef, own_jacobi, diag = pl.pallas_call(
        prepare_kernel,
        out_shape=(
            bf16(5 * values, 2 * values),
            bf16(CHILDREN * values, 2 * values),
            bf16(2 * values, CHILDREN * values),
            f32(capacity, values),
            f32(capacity, values),
            f32(8, values),
        ),
        in_specs=[vmem] * 5,
        out_specs=(vmem,) * 6,
        name="prepare",
    )(cell_matrix, face_near, face_far, prolong, cell_coef.reshape(capacity // values, values))
    iterate, residual, coef, jacobi, message = pl.pallas_call(
        fine_kernel,
        out_shape=(f32(frame, values),) * 4 + (f32(slots + 2 * margin + 8, values),),
        in_specs=[smem] + [vmem] * 8,
        out_specs=(vmem,) * 5,
        scratch_shapes=[buffer(frame, values), buffer(values, values)],
        name="fine",
    )(fine_count, right_side, first_in, second_in, coupling, restrict, own_coef, own_jacobi, diag)
    one_a = exchange(message, 1, 0)
    one_b = exchange(message, 1, 1)
    two_a = exchange(message, 2, 0)
    two_b = exchange(message, 2, 1)
    device = device_number()
    is_even = device % 2 == 0
    is_low = device % 4 < 2
    before_one = jnp.where(is_even, one_b, one_a)
    after_one = jnp.where(is_even, one_a, one_b)
    before_two = jnp.where(is_low, two_b, two_a)
    after_two = jnp.where(is_low, two_a, two_b)
    coarse_frame = 5 * slots + 3 * margin
    return pl.pallas_call(
        coarse_kernel,
        out_shape=f32(capacity, values),
        in_specs=[smem] + [vmem] * 12,
        out_specs=vmem,
        scratch_shapes=[buffer(frame, values)] + [buffer(coarse_frame, values)] * 5 + [buffer(frame, values)],
        name="coarse",
    )(
        fine_count, iterate, residual, coef, jacobi, message, before_one, before_two, after_one, after_two,
        coupling, spread, diag,
    )


def solution(mesh):
    placed = (P(AXES, None), P(AXES), P(), P(), P(), P(), P())
    return jax.shard_map(
        shards, mesh=mesh, in_specs=placed, out_specs=P(AXES, None), check_vma=False
    )
```

```python
import jax
import jax.numpy as jnp
from jax import lax
from jax.experimental import pallas as pl
from jax.experimental.pallas import tpu as pltpu
from jax.sharding import PartitionSpec as P

DEG = 3
AXES = ("sfc", "lvl")
CENTER = 1.025
RADIUS = 0.775
CHILDREN = 8
GRANT = 16 * 1024 * 1024


def chebyshev_weights():
    sigma = CENTER / RADIUS
    weight = 1.0 / sigma
    steps = [(0.0, 1.0 / CENTER)]
    for _ in range(DEG - 1):
        following = 1.0 / (2.0 * sigma - weight)
        steps.append((following * weight, 2.0 * following / RADIUS))
        weight = following
    return steps


STEPS = chebyshev_weights()


def step_weights(step):
    keep = jnp.float32(STEPS[0][0])
    gain = jnp.float32(STEPS[0][1])
    for index in range(1, DEG):
        keep = jnp.where(step == index, jnp.float32(STEPS[index][0]), keep)
        gain = jnp.where(step == index, jnp.float32(STEPS[index][1]), gain)
    return keep, gain


def device_number():
    return lax.axis_index("sfc") * lax.axis_size("lvl") + lax.axis_index("lvl")


def device_total():
    return lax.axis_size("sfc") * lax.axis_size("lvl")


def halves(value):
    high = value.astype(jnp.bfloat16)
    low = (value - high.astype(jnp.float32)).astype(jnp.bfloat16)
    return high, low


def dot(left, right):
    return jnp.dot(left, right, preferred_element_type=jnp.float32)


def product(parts, pair):
    width = pair.shape[1] // 2
    split = [halves(part) for part in parts]
    high = jnp.concatenate([one[0] for one in split], 1)
    low = jnp.concatenate([one[1] for one in split], 1)
    both = dot(high, pair[...])
    return both[:, :width] + both[:, width:] + dot(low, pair[:, :width])


def neighbours(field, start, rows, stride):
    return [field[pl.ds(start + shift, rows), :] for shift in (0, 1, -1, stride, -stride)]


def columns(row, lanes):
    return jnp.transpose(jnp.broadcast_to(row, (lanes, lanes)))


def pack_kernel(count, right_side, coef, first, second, turned):
    values = right_side.shape[1]
    depth = first.shape[0] - 8
    device = device_number()
    live = count[device]
    is_even = device % 2 == 0
    spare = jnp.ones((8 - coef.shape[0], values), jnp.float32)
    rows_of_coef = jnp.concatenate([coef[...], spare], 0)
    tail = pl.multiple_of(live - depth, 8)
    for out, start in (
        (first, jnp.where(is_even, tail, 0)),
        (second, jnp.where(is_even, 0, tail)),
    ):
        start = pl.multiple_of(start, 8)
        out[:depth, :] = right_side[pl.ds(start, depth), :]
        row = start // values
        lane = start % values
        turned[:8, :] = pltpu.roll(rows_of_coef, (values - lane) % values, 1)
        lanes = lax.broadcasted_iota(jnp.int32, (8, values), 1)
        near = turned[pl.ds(row, 8), :]
        far = turned[pl.ds(row + 1, 8), :]
        out[depth:, :] = jnp.where(lanes < values - lane, near, far)


def prepare_kernel(
    cell_matrix, face_near, face_far, prolong, coef, coupling, restrict, spread, own_coef, own_jacobi, diag
):
    values = cell_matrix.shape[0]
    near = face_near[...]
    far = face_far[...]
    blocks = (cell_matrix[...], -near, -jnp.transpose(near), -far, -jnp.transpose(far))
    for index, block in enumerate(blocks):
        rows = pl.ds(index * values, values)
        high, low = halves(block)
        coupling[rows, :values] = high
        coupling[rows, values:] = low
    for child in range(CHILDREN):
        rows = pl.ds(child * values, values)
        block = prolong[child]
        high, low = halves(block)
        spread[:values, rows] = high
        spread[values:, rows] = low
        high, low = halves(jnp.transpose(block))
        restrict[rows, :values] = high
        restrict[rows, values:] = low
    row_index = lax.broadcasted_iota(jnp.int32, (values, values), 0)
    lane_index = lax.broadcasted_iota(jnp.int32, (values, values), 1)
    diagonal = jnp.sum(
        jnp.where(row_index == lane_index, cell_matrix[...], 0.0), axis=0, keepdims=True
    )
    diag[...] = jnp.broadcast_to(diagonal, diag.shape)
    for row in range(coef.shape[0]):
        rows = pl.ds(row * values, values)
        column = columns(coef[row : row + 1, :], values)
        own_coef[rows, :] = column
        own_jacobi[rows, :] = 1.0 / (column + diagonal)


def fine_kernel(
    count, right_side, first, second, coupling, restrict, own_coef, own_jacobi, diag,
    iterate, residual, coef, jacobi, message, update, coarse_coef,
):
    capacity, values = right_side.shape
    stride = capacity // 16
    depth = first.shape[0] - 8
    frame = capacity + 2 * depth
    device = device_number()
    total = device_total()
    live = count[device]
    is_even = device % 2 == 0
    end = pl.multiple_of(depth + live, 8)
    left = jnp.where(is_even, second[...], first[...])
    right = jnp.where(is_even, first[...], second[...])
    diagonal = diag[0:1, :]

    def column_of(side):
        pieces = []
        for row in range(-(-depth // values)):
            pieces.append(columns(side[depth + row : depth + row + 1, :], values))
        return jnp.concatenate(pieces, 0)[:depth]

    left_coef = column_of(left)
    right_coef = column_of(right)
    residual[:depth, :] = left[:depth]
    residual[pl.ds(depth, capacity), :] = right_side[...]
    residual[pl.ds(depth + capacity, depth), :] = jnp.zeros((depth, values), jnp.float32)
    residual[pl.ds(end, depth), :] = right[:depth]
    coef[:depth, :] = left_coef
    coef[pl.ds(depth, capacity), :] = own_coef[...]
    coef[pl.ds(depth + capacity, depth), :] = jnp.zeros((depth, values), jnp.float32)
    coef[pl.ds(end, depth), :] = right_coef
    jacobi[:depth, :] = jnp.where(device > 0, 1.0 / (left_coef + diagonal), 0.0)
    jacobi[pl.ds(depth, capacity), :] = own_jacobi[...]
    jacobi[pl.ds(depth + capacity, depth), :] = jnp.zeros((depth, values), jnp.float32)
    jacobi[pl.ds(end, depth), :] = jnp.where(device < total - 1, 1.0 / (right_coef + diagonal), 0.0)
    update[...] = jnp.zeros(update.shape, jnp.float32)
    iterate[...] = jnp.zeros(iterate.shape, jnp.float32)

    def step(index, carry):
        keep, gain = step_weights(index)
        fresh = keep * update[...] + gain * (jacobi[...] * residual[...])
        update[...] = fresh
        iterate[...] += fresh
        span = (frame - 2 * stride) // 2
        for block in range(2):
            start = stride + block * span
            rows = pl.ds(start, span)
            applied = product(neighbours(update, start, span, stride), coupling)
            residual[rows, :] = residual[rows, :] - (coef[rows, :] * update[rows, :] + applied)
        return carry

    lax.fori_loop(0, DEG, step, 0)
    cells = message.shape[0] - 8
    first_row = depth - CHILDREN * ((cells - capacity // CHILDREN) // 2)
    parts = [residual[pl.ds(first_row + c, cells, stride=CHILDREN), :] for c in range(CHILDREN)]
    message[:cells, :] = product(parts, restrict)
    mean = coef[pl.ds(first_row, cells, stride=CHILDREN), :]
    for c in range(1, CHILDREN):
        mean = mean + coef[pl.ds(first_row + c, cells, stride=CHILDREN), :]
    coarse_coef[...] = jnp.zeros(coarse_coef.shape, jnp.float32)
    coarse_coef[:cells, :] = mean * (1.0 / CHILDREN)
    message[cells:, :] = jnp.transpose(coarse_coef[...])[:8]


def coarse_kernel(
    count, iterate, residual, coef, jacobi, own, one_a, one_b, two_a, two_b,
    coupling, spread, diag, out, solved, source, coarse_coef, coarse_jacobi, coarse_update, coarse, update,
):
    capacity, values = out.shape
    stride = capacity // 16
    slots = capacity // CHILDREN
    margin = (own.shape[0] - 8 - slots) // 2
    depth = (iterate.shape[0] - capacity) // 2
    reach = depth // 2 // CHILDREN
    base = 2 * slots + margin
    device = device_number()
    total = device_total()

    def cells_of(offset):
        at = device + offset
        inside = (at >= 0) & (at < total)
        return jnp.where(inside, count[jnp.clip(at, 0, total - 1)] // CHILDREN, 0)

    size = cells_of(0)
    start_before = base - cells_of(-1)
    start_after = base + size
    start_last = start_after + cells_of(1)
    source[...] = jnp.zeros(source.shape, jnp.float32)
    coarse_coef[...] = jnp.zeros(coarse_coef.shape, jnp.float32)
    is_even = device % 2 == 0
    is_low = device % 4 < 2
    before_one = jnp.where(is_even, one_b[...], one_a[...])
    after_one = jnp.where(is_even, one_a[...], one_b[...])
    before_two = jnp.where(is_low, two_b[...], two_a[...])
    after_two = jnp.where(is_low, two_a[...], two_b[...])
    placed = (
        (before_two, start_before - cells_of(-2) - margin, 0, slots + 2 * margin),
        (before_one, start_before, margin, slots),
        (own, base, margin, slots),
        (after_one, start_after, margin, slots),
        (after_two, start_last, margin, slots + margin),
    )
    for piece, at, begin, rows in placed:
        source[pl.ds(at, rows), :] = piece[begin : begin + rows, :]
        column = columns(piece[slots + 2 * margin : slots + 2 * margin + 1, :], values)
        coarse_coef[pl.ds(at, rows), :] = column[begin : begin + rows]
    lowest = start_before - cells_of(-2) - jnp.where(device > 2, margin, 0)
    highest = start_last + cells_of(2) + jnp.where(device < total - 3, margin, 0)
    row_index = lax.broadcasted_iota(jnp.int32, source.shape, 0)
    inside = (row_index >= lowest) & (row_index < highest)
    coarse_jacobi[...] = jnp.where(inside, 1.0 / (coarse_coef[...] + diag[0:1, :]), 0.0)
    fresh = STEPS[0][1] * (coarse_jacobi[...] * source[...])
    coarse_update[...] = fresh
    coarse[...] = fresh
    low = base - slots - margin
    high = base + 2 * slots + margin
    for index in range(1, DEG):
        keep, gain = STEPS[index]
        rows = pl.ds(low, high - low)
        applied = product(neighbours(coarse_update, low, high - low, stride), coupling)
        source[rows, :] = source[rows, :] - (coarse_coef[rows, :] * coarse_update[rows, :] + applied)
        fresh = keep * coarse_update[rows, :] + gain * (coarse_jacobi[rows, :] * source[rows, :])
        coarse_update[rows, :] = fresh
        coarse[rows, :] += fresh
    count_rows = slots + 2 * reach
    correction = coarse[pl.ds(base - reach, count_rows), :]
    high_part, low_part = halves(correction)
    spread_high = spread[:values, :]
    children = dot(high_part, spread_high) + dot(low_part, spread_high) + dot(high_part, spread[values:, :])
    first_row = depth - CHILDREN * reach
    for c in range(CHILDREN):
        update[pl.ds(first_row + c, count_rows, stride=CHILDREN), :] = children[:, c * values : (c + 1) * values]
    used = pl.ds(first_row, CHILDREN * count_rows)
    solved[used, :] = iterate[used, :] + update[used, :]
    work = pl.ds(first_row, CHILDREN * count_rows)
    update[pl.ds(first_row - stride, stride), :] = jnp.zeros((stride, values), jnp.float32)
    update[pl.ds(first_row + CHILDREN * count_rows, stride), :] = jnp.zeros((stride, values), jnp.float32)
    solved_residual = residual

    def step(index, carry):
        keep, gain = step_weights(index)
        span = (CHILDREN * count_rows - 2 * stride) // 2
        for block in range(2):
            start = first_row + stride + block * span
            rows = pl.ds(start, span)
            applied = product(neighbours(update, start, span, stride), coupling)
            solved_residual[rows, :] = solved_residual[rows, :] - (coef[rows, :] * update[rows, :] + applied)
        fresh = keep * update[work, :] + gain * (jacobi[work, :] * solved_residual[work, :])
        update[work, :] = fresh
        solved[work, :] += fresh
        return carry

    lax.fori_loop(0, DEG, step, 0)
    live = count[device]
    is_live = lax.broadcasted_iota(jnp.int32, (capacity, values), 0) < live
    out[...] = jnp.where(is_live, solved[pl.ds(depth, capacity), :], 0.0)


def exchange(block, distance, phase):
    total = lax.axis_size(AXES)
    pairs = []
    for device in range(total - distance):
        if (device // distance) % 2 == phase:
            pairs += [(device, device + distance), (device + distance, device)]
    return lax.ppermute(block, AXES, pairs)


def shards(right_side, cell_coef, fine_count, cell_matrix, face_near, face_far, prolong):
    capacity, values = right_side.shape
    stride = capacity // 16
    depth = 6 * stride
    frame = capacity + 2 * depth
    slots = capacity // CHILDREN
    margin = 16
    coef_rows = cell_coef.reshape(capacity // values, values)
    f32 = lambda *shape: jax.ShapeDtypeStruct(shape, jnp.float32)
    bf16 = lambda *shape: jax.ShapeDtypeStruct(shape, jnp.bfloat16)
    buffer = lambda *shape: pltpu.VMEM(shape, jnp.float32)
    smem = pl.BlockSpec(memory_space=pltpu.SMEM)
    vmem = pl.BlockSpec(memory_space=pltpu.VMEM)

    first, second = pl.pallas_call(
        pack_kernel,
        out_shape=(f32(depth + 8, values), f32(depth + 8, values)),
        in_specs=[smem, vmem, vmem],
        out_specs=(vmem, vmem),
        scratch_shapes=[buffer(24, values)],
        name="pack",
        compiler_params=pltpu.CompilerParams(vmem_limit_bytes=GRANT),
    )(fine_count, right_side, coef_rows)
    second_in = exchange(second, 1, 1)
    first_in = exchange(first, 1, 0)
    coupling, restrict, spread, own_coef, own_jacobi, diag = pl.pallas_call(
        prepare_kernel,
        out_shape=(
            bf16(5 * values, 2 * values),
            bf16(CHILDREN * values, 2 * values),
            bf16(2 * values, CHILDREN * values),
            f32(capacity, values),
            f32(capacity, values),
            f32(8, values),
        ),
        in_specs=[vmem] * 5,
        out_specs=(vmem,) * 6,
        name="prepare",
        compiler_params=pltpu.CompilerParams(vmem_limit_bytes=GRANT),
    )(cell_matrix, face_near, face_far, prolong, coef_rows)
    iterate, residual, coef, jacobi, message = pl.pallas_call(
        fine_kernel,
        out_shape=(f32(frame, values),) * 4 + (f32(slots + 2 * margin + 8, values),),
        in_specs=[smem] + [vmem] * 8,
        out_specs=(vmem,) * 5,
        scratch_shapes=[buffer(frame, values), buffer(values, values)],
        name="fine",
        compiler_params=pltpu.CompilerParams(vmem_limit_bytes=GRANT),
    )(fine_count, right_side, first_in, second_in, coupling, restrict, own_coef, own_jacobi, diag)
    one_b = exchange(message, 1, 1)
    two_b = exchange(message, 2, 1)
    one_a = exchange(message, 1, 0)
    two_a = exchange(message, 2, 0)
    coarse_frame = 5 * slots + 3 * margin
    return pl.pallas_call(
        coarse_kernel,
        out_shape=f32(capacity, values),
        in_specs=[smem] + [vmem] * 12,
        out_specs=vmem,
        scratch_shapes=[buffer(frame, values)] + [buffer(coarse_frame, values)] * 5 + [buffer(frame, values)],
        name="coarse",
        compiler_params=pltpu.CompilerParams(vmem_limit_bytes=GRANT),
    )(
        fine_count, iterate, residual, coef, jacobi, message, one_a, one_b, two_a, two_b,
        coupling, spread, diag,
    )


def solution(mesh):
    placed = (P(AXES, None), P(AXES), P(), P(), P(), P(), P())
    return jax.shard_map(
        shards, mesh=mesh, in_specs=placed, out_specs=P(AXES, None), check_vma=False
    )
```

```python
import jax
import jax.numpy as jnp
from jax import lax
from jax.experimental import pallas as pl
from jax.experimental.pallas import tpu as pltpu
from jax.sharding import PartitionSpec as P

DEG = 3
AXES = ("sfc", "lvl")
CENTER = 1.025
RADIUS = 0.775
CHILDREN = 8
NEAR_CELLS = 2
GRANT = 16 * 1024 * 1024


def chebyshev_weights():
    sigma = CENTER / RADIUS
    weight = 1.0 / sigma
    steps = [(0.0, 1.0 / CENTER)]
    for _ in range(DEG - 1):
        following = 1.0 / (2.0 * sigma - weight)
        steps.append((following * weight, 2.0 * following / RADIUS))
        weight = following
    return steps


STEPS = chebyshev_weights()


def device_number():
    return lax.axis_index("sfc") * lax.axis_size("lvl") + lax.axis_index("lvl")


def device_total():
    return lax.axis_size("sfc") * lax.axis_size("lvl")


def halves(value):
    high = value.astype(jnp.bfloat16)
    low = (value - high.astype(jnp.float32)).astype(jnp.bfloat16)
    return high, low


def dot(left, right):
    return jnp.dot(left, right, preferred_element_type=jnp.float32)


def product(parts, pair):
    width = pair.shape[1] // 2
    split = [halves(part) for part in parts]
    high = jnp.concatenate([one[0] for one in split], 1)
    low = jnp.concatenate([one[1] for one in split], 1)
    both = dot(high, pair[...])
    return both[:, :width] + both[:, width:] + dot(low, pair[:, :width])


def neighbours(field, start, rows, stride):
    return [field[pl.ds(start + shift, rows), :] for shift in (0, 1, -1, stride, -stride)]


def columns(row, lanes):
    return jnp.transpose(jnp.broadcast_to(row, (lanes, lanes)))


def scalar_of(numbers, index):
    return numbers[index : index + 1, 0:1][0, 0]


def pack_kernel(count_in, right_in, coef_in, first, second, numbers, count, right_side, coef, turned, arrivals):
    values = right_side.shape[1]
    depth = first.shape[0] - 8
    copies = (
        pltpu.make_async_copy(count_in, count, arrivals.at[0]),
        pltpu.make_async_copy(right_in, right_side, arrivals.at[1]),
        pltpu.make_async_copy(coef_in, coef.at[pl.ds(0, coef_in.shape[0])], arrivals.at[2]),
    )
    for copy in copies:
        copy.start()
    device = device_number()
    total = device_total()
    coef[pl.ds(coef_in.shape[0], 8 - coef_in.shape[0]), :] = jnp.ones(
        (8 - coef_in.shape[0], values), jnp.float32
    )
    turned[...] = jnp.ones(turned.shape, jnp.float32)
    copies[0].wait()
    rows = lax.broadcasted_iota(jnp.int32, numbers.shape, 0)
    table = jnp.zeros(numbers.shape, jnp.int32)
    for offset in range(-NEAR_CELLS, NEAR_CELLS + 1):
        at = device + offset
        size = jnp.where((at >= 0) & (at < total), count[jnp.clip(at, 0, total - 1)], 0)
        table = jnp.where(rows == offset + NEAR_CELLS, size, table)
    numbers[...] = table
    live = count[device]
    is_even = device % 2 == 0
    tail = live - depth
    copies[2].wait()
    for out, start in (
        (first, jnp.where(is_even, tail, 0)),
        (second, jnp.where(is_even, 0, tail)),
    ):
        row = start // values
        lane = start % values
        turned[:8, :] = pltpu.roll(coef[...], (values - lane) % values, 1)
        lanes = lax.broadcasted_iota(jnp.int32, (8, values), 1)
        near = turned[pl.ds(row, 8), :]
        far = turned[pl.ds(row + 1, 8), :]
        out[depth:, :] = jnp.where(lanes < values - lane, near, far)
    copies[1].wait()
    for out, start in (
        (first, jnp.where(is_even, tail, 0)),
        (second, jnp.where(is_even, 0, tail)),
    ):
        out[:depth, :] = right_side[pl.ds(pl.multiple_of(start, 8), depth), :]


def interior_kernel(
    numbers, right_in, coef_in, cell_in, near_in, far_in, prolong_in,
    coupling, restrict, spread, diag, residual, coef, jacobi, *rest,
):
    updates = rest[:DEG]
    coef_rows, cell_matrix, face_near, face_far, prolong, arrivals = rest[DEG:]
    values = cell_in.shape[0]
    capacity = right_in.shape[0]
    stride = capacity // 16
    depth = (residual.shape[0] - capacity) // 2
    right_side = residual.at[pl.ds(depth, capacity)]
    copies = [
        pltpu.make_async_copy(origin, target, arrivals.at[index])
        for index, (origin, target) in enumerate(
            (
                (cell_in, cell_matrix),
                (near_in, face_near),
                (far_in, face_far),
                (coef_in, coef_rows),
                (right_in, right_side),
                (prolong_in, prolong),
            )
        )
    ]
    for copy in copies:
        copy.start()
    spare = pl.ds(depth + capacity, depth)
    for field in (residual, coef, jacobi) + updates:
        field[spare, :] = jnp.zeros((depth, values), jnp.float32)
    for copy in copies[:5]:
        copy.wait()
    near = face_near[...]
    far = face_far[...]
    blocks = (cell_matrix[...], -near, -jnp.transpose(near), -far, -jnp.transpose(far))
    for index, block in enumerate(blocks):
        rows = pl.ds(index * values, values)
        high, low = halves(block)
        coupling[rows, :values] = high
        coupling[rows, values:] = low
    row_index = lax.broadcasted_iota(jnp.int32, (values, values), 0)
    lane_index = lax.broadcasted_iota(jnp.int32, (values, values), 1)
    diagonal = jnp.sum(
        jnp.where(row_index == lane_index, cell_matrix[...], 0.0), axis=0, keepdims=True
    )
    diag[...] = jnp.broadcast_to(diagonal, diag.shape)
    keep, gain = STEPS[0]
    for row in range(capacity // values):
        rows = pl.ds(depth + row * values, values)
        column = columns(coef_rows[row : row + 1, :], values)
        source = residual[rows, :]
        scale = 1.0 / (column + diagonal)
        coef[rows, :] = column
        jacobi[rows, :] = scale
        updates[0][rows, :] = gain * (scale * source)
    end = depth + scalar_of(numbers, NEAR_CELLS)
    for index in range(1, DEG + 1):
        start = depth + index * stride
        span = capacity - 2 * index * stride
        rows = pl.ds(start, span)
        before = updates[index - 1]
        old = residual[rows, :]
        fresh = old - (
            coef[rows, :] * before[rows, :] + product(neighbours(before, start, span, stride), coupling)
        )
        inside = start + lax.broadcasted_iota(jnp.int32, (span, values), 0) < end - index * stride
        residual[rows, :] = jnp.where(inside, fresh, old)
        if index < DEG:
            keep, gain = STEPS[index]
            updates[index][rows, :] = keep * before[rows, :] + gain * (jacobi[rows, :] * fresh)
    copies[5].wait()
    for child in range(CHILDREN):
        rows = pl.ds(child * values, values)
        block = prolong[child]
        high, low = halves(block)
        spread[:values, rows] = high
        spread[values:, rows] = low
        high, low = halves(jnp.transpose(block))
        restrict[rows, :values] = high
        restrict[rows, values:] = low


def boundary_kernel(
    numbers, first, second, coupling, restrict, diag, *fields
):
    residual, coef, jacobi = fields[DEG + 3 : DEG + 6]
    updates = fields[DEG + 6 : 2 * DEG + 6]
    message, coarse_coef = fields[2 * DEG + 6 :]
    frame, values = residual.shape
    depth = first.shape[0] - 8
    capacity = frame - 2 * depth
    stride = capacity // 16
    device = device_number()
    total = device_total()
    is_even = device % 2 == 0
    end = pl.multiple_of(depth + scalar_of(numbers, NEAR_CELLS), 8)
    diagonal = diag[0:1, :]
    left = jnp.where(is_even, second[...], first[...])
    right = jnp.where(is_even, first[...], second[...])
    keep, gain = STEPS[0]
    for side, start, exists in ((left, 0, device > 0), (right, end, device < total - 1)):
        pieces = []
        for row in range(-(-depth // values)):
            pieces.append(columns(side[depth + row : depth + row + 1, :], values))
        column = jnp.concatenate(pieces, 0)[:depth]
        scale = jnp.where(exists, 1.0 / (column + diagonal), 0.0)
        rows = pl.ds(start, depth)
        residual[rows, :] = side[:depth]
        coef[rows, :] = column
        jacobi[rows, :] = scale
        updates[0][rows, :] = gain * (scale * side[:depth])
    for index in range(1, DEG + 1):
        before = updates[index - 1]
        starts = (index * stride, pl.multiple_of(end - index * stride, 8))
        parts = [
            jnp.concatenate([before[pl.ds(start + shift, depth), :] for start in starts], 0)
            for shift in (0, 1, -1, stride, -stride)
        ]
        applied = product(parts, coupling)
        for side, start in enumerate(starts):
            rows = pl.ds(start, depth)
            own = parts[0][side * depth : (side + 1) * depth]
            fresh = residual[rows, :] - (coef[rows, :] * own + applied[side * depth : (side + 1) * depth])
            residual[rows, :] = fresh
            if index < DEG:
                keep, gain = STEPS[index]
                updates[index][rows, :] = keep * own + gain * (jacobi[rows, :] * fresh)
    cells = message.shape[0] - 8
    first_row = depth - CHILDREN * ((cells - capacity // CHILDREN) // 2)
    parts = [residual[pl.ds(first_row + c, cells, stride=CHILDREN), :] for c in range(CHILDREN)]
    message[:cells, :] = product(parts, restrict)
    mean = coef[pl.ds(first_row, cells, stride=CHILDREN), :]
    for c in range(1, CHILDREN):
        mean = mean + coef[pl.ds(first_row + c, cells, stride=CHILDREN), :]
    coarse_coef[...] = jnp.zeros(coarse_coef.shape, jnp.float32)
    coarse_coef[:cells, :] = mean * (1.0 / CHILDREN)
    message[cells:, :] = jnp.transpose(coarse_coef[...])[:8]


def coarse_kernel(
    numbers, residual, coef, jacobi, *rest
):
    presmoothed = rest[:DEG]
    own, one_a, one_b, two_a, two_b, coupling, spread, diag, out_hbm = rest[DEG : DEG + 9]
    source, coarse_coef, coarse_jacobi = rest[DEG + 9 : DEG + 12]
    coarse_updates = rest[DEG + 12 : 2 * DEG + 12]
    updates = rest[2 * DEG + 12 : 3 * DEG + 12]
    out, sent = rest[3 * DEG + 12 :]
    capacity, values = out.shape
    stride = capacity // 16
    slots = capacity // CHILDREN
    margin = (own.shape[0] - 8 - slots) // 2
    depth = (residual.shape[0] - capacity) // 2
    reach = depth // 2 // CHILDREN
    base = 2 * slots + margin
    device = device_number()
    total = device_total()

    def cells_of(offset):
        return scalar_of(numbers, NEAR_CELLS + offset) // CHILDREN

    start_before = base - cells_of(-1)
    start_first = start_before - cells_of(-2)
    start_after = base + cells_of(0)
    start_last = start_after + cells_of(1)
    source[...] = jnp.zeros(source.shape, jnp.float32)
    coarse_coef[...] = jnp.zeros(coarse_coef.shape, jnp.float32)
    is_even = device % 2 == 0
    is_low = device % 4 < 2
    before_one = jnp.where(is_even, one_b[...], one_a[...])
    after_one = jnp.where(is_even, one_a[...], one_b[...])
    before_two = jnp.where(is_low, two_b[...], two_a[...])
    after_two = jnp.where(is_low, two_a[...], two_b[...])
    placed = (
        (before_two, start_first - margin, 0, slots + 2 * margin),
        (before_one, start_before, margin, slots),
        (own, base, margin, slots),
        (after_one, start_after, margin, slots),
        (after_two, start_last, margin, slots + margin),
    )
    for piece, at, begin, rows in placed:
        source[pl.ds(at, rows), :] = piece[begin : begin + rows, :]
        column = columns(piece[slots + 2 * margin : slots + 2 * margin + 1, :], values)
        coarse_coef[pl.ds(at, rows), :] = column[begin : begin + rows]
    lowest = start_first - jnp.where(device > 2, margin, 0)
    highest = start_last + cells_of(2) + jnp.where(device < total - 3, margin, 0)
    row_index = lax.broadcasted_iota(jnp.int32, source.shape, 0)
    inside = (row_index >= lowest) & (row_index < highest)
    coarse_jacobi[...] = jnp.where(inside, 1.0 / (coarse_coef[...] + diag[0:1, :]), 0.0)
    coarse_updates[0][...] = STEPS[0][1] * (coarse_jacobi[...] * source[...])
    for index in range(1, DEG):
        keep, gain = STEPS[index]
        before = coarse_updates[index - 1]
        start = base - margin - (DEG - 1 - index) * stride
        span = slots + 2 * margin + 2 * (DEG - 1 - index) * stride
        rows = pl.ds(start, span)
        own_update = before[rows, :]
        fresh = source[rows, :] - (
            coarse_coef[rows, :] * own_update + product(neighbours(before, start, span, stride), coupling)
        )
        source[rows, :] = fresh
        coarse_updates[index][rows, :] = keep * own_update + gain * (coarse_jacobi[rows, :] * fresh)
    count_rows = slots + 2 * reach
    rows = pl.ds(base - reach, count_rows)
    correction = coarse_updates[0][rows, :]
    for index in range(1, DEG):
        correction = correction + coarse_updates[index][rows, :]
    high_part, low_part = halves(correction)
    spread_high = spread[:values, :]
    children = dot(high_part, spread_high) + dot(low_part, spread_high) + dot(high_part, spread[values:, :])
    first_row = depth - CHILDREN * reach
    for c in range(CHILDREN):
        updates[0][pl.ds(first_row + c, count_rows, stride=CHILDREN), :] = children[:, c * values : (c + 1) * values]
    for index in range(DEG):
        keep, gain = STEPS[index]
        before = updates[index]
        begin = first_row + (index + 1) * stride
        span = (CHILDREN * count_rows - 2 * (index + 1) * stride) // 2
        for block in range(2):
            start = begin + block * span
            rows = pl.ds(start, span)
            own_update = before[rows, :]
            fresh = residual[rows, :] - (
                coef[rows, :] * own_update + product(neighbours(before, start, span, stride), coupling)
            )
            step = gain * (jacobi[rows, :] * fresh)
            if index > 0:
                step = step + keep * own_update
            if index < DEG - 1:
                residual[rows, :] = fresh
                updates[index + 1][rows, :] = step
            else:
                total_update = step
                for field in presmoothed + updates:
                    total_update = total_update + field[rows, :]
                slot = start - depth
                is_live = slot + lax.broadcasted_iota(jnp.int32, (span, values), 0) < scalar_of(numbers, NEAR_CELLS)
                out[pl.ds(slot, span), :] = jnp.where(is_live, total_update, 0.0)
                pltpu.make_async_copy(
                    out.at[pl.ds(slot, span)], out_hbm.at[pl.ds(slot, span)], sent.at[block]
                ).start()
    for block in range(2):
        piece = pl.ds(block * (capacity // 2), capacity // 2)
        pltpu.make_async_copy(out.at[piece], out_hbm.at[piece], sent.at[block]).wait()


def exchange(block, distance, phase, complete):
    total = lax.axis_size(AXES)
    pairs = []
    for device in range(total - distance):
        if (device // distance) % 2 == phase:
            pairs += [(device, device + distance), (device + distance, device)]
    if complete:
        busy = {source for source, _ in pairs}
        idle = [device for device in range(total) if device not in busy]
        for one, other in zip(idle[0::2], idle[1::2]):
            pairs += [(one, other), (other, one)]
    return lax.ppermute(block, AXES, pairs)


def shards(right_side, cell_coef, fine_count, cell_matrix, face_near, face_far, prolong):
    capacity, values = right_side.shape
    stride = capacity // 16
    depth = 2 * DEG * stride
    frame = capacity + 2 * depth
    slots = capacity // CHILDREN
    margin = 16
    coef_rows = cell_coef.reshape(capacity // values, values)
    f32 = lambda *shape: jax.ShapeDtypeStruct(shape, jnp.float32)
    bf16 = lambda *shape: jax.ShapeDtypeStruct(shape, jnp.bfloat16)
    buffer = lambda *shape: pltpu.VMEM(shape, jnp.float32)
    vmem = pl.BlockSpec(memory_space=pltpu.VMEM)
    hbm = pl.BlockSpec(memory_space=pltpu.HBM)
    params = pltpu.CompilerParams(vmem_limit_bytes=GRANT)
    off_chip = lambda array: pltpu.with_memory_space_constraint(array, pltpu.HBM)

    first, second, numbers = pl.pallas_call(
        pack_kernel,
        out_shape=(
            f32(depth + 8, values),
            f32(depth + 8, values),
            jax.ShapeDtypeStruct((8, values), jnp.int32),
        ),
        in_specs=[hbm, hbm, hbm],
        out_specs=(vmem, vmem, vmem),
        scratch_shapes=[
            pltpu.SMEM(fine_count.shape, jnp.int32),
            buffer(capacity, values),
            buffer(8, values),
            buffer(24, values),
            pltpu.SemaphoreType.DMA((3,)),
        ],
        name="pack",
        compiler_params=params,
    )(off_chip(fine_count), off_chip(right_side), off_chip(coef_rows))
    second_in = exchange(second, 1, 1, True)
    first_in = exchange(first, 1, 0, False)
    prepared = pl.pallas_call(
        interior_kernel,
        out_shape=(
            bf16(5 * values, 2 * values),
            bf16(CHILDREN * values, 2 * values),
            bf16(2 * values, CHILDREN * values),
            f32(8, values),
        )
        + (f32(frame, values),) * (3 + DEG),
        in_specs=[vmem] + [hbm] * 6,
        out_specs=(vmem,) * (7 + DEG),
        scratch_shapes=[
            buffer(*coef_rows.shape),
            buffer(values, values),
            buffer(values, values),
            buffer(values, values),
            buffer(*prolong.shape),
            pltpu.SemaphoreType.DMA((6,)),
        ],
        name="interior",
        compiler_params=params,
    )(numbers, *(off_chip(each) for each in (right_side, coef_rows, cell_matrix, face_near, face_far, prolong)))
    coupling, restrict, spread, diag = prepared[:4]
    *fields, message = pl.pallas_call(
        boundary_kernel,
        out_shape=(f32(frame, values),) * (3 + DEG) + (f32(slots + 2 * margin + 8, values),),
        in_specs=[vmem] * (9 + DEG),
        out_specs=(vmem,) * (4 + DEG),
        scratch_shapes=[buffer(values, values)],
        input_output_aliases={6 + index: index for index in range(3 + DEG)},
        name="boundary",
        compiler_params=params,
    )(numbers, first_in, second_in, coupling, restrict, diag, *prepared[4:])
    one_b = exchange(message, 1, 1, False)
    two_b = exchange(message, 2, 1, True)
    one_a = exchange(message, 1, 0, False)
    two_a = exchange(message, 2, 0, False)
    coarse_frame = 5 * slots + 3 * margin
    return pl.pallas_call(
        coarse_kernel,
        out_shape=f32(capacity, values),
        in_specs=[vmem] * (4 + DEG + 8),
        out_specs=hbm,
        scratch_shapes=[buffer(coarse_frame, values)] * (3 + DEG)
        + [buffer(frame, values)] * DEG
        + [buffer(capacity, values), pltpu.SemaphoreType.DMA((2,))],
        name="coarse",
        compiler_params=params,
    )(numbers, *fields, message, one_a, one_b, two_a, two_b, coupling, spread, diag)


def solution(mesh):
    placed = (P(AXES, None), P(AXES), P(), P(), P(), P(), P())
    return jax.shard_map(
        shards, mesh=mesh, in_specs=placed, out_specs=P(AXES, None), check_vma=False
    )
```

```python
import jax
import jax.numpy as jnp
from jax import lax
from jax.experimental import pallas as pl
from jax.experimental.pallas import tpu as pltpu
from jax.sharding import PartitionSpec as P

DEG = 3
AXES = ("sfc", "lvl")
CENTER = 1.025
RADIUS = 0.775
CHILDREN = 8
NEAR_CELLS = 2
GRANT = 16 * 1024 * 1024


def chebyshev_weights():
    sigma = CENTER / RADIUS
    weight = 1.0 / sigma
    steps = [(0.0, 1.0 / CENTER)]
    for _ in range(DEG - 1):
        following = 1.0 / (2.0 * sigma - weight)
        steps.append((following * weight, 2.0 * following / RADIUS))
        weight = following
    return steps


STEPS = chebyshev_weights()


def device_number():
    return lax.axis_index("sfc") * lax.axis_size("lvl") + lax.axis_index("lvl")


def device_total():
    return lax.axis_size("sfc") * lax.axis_size("lvl")


def is_near_end(device, total):
    return (device == 1) | (device == 2) | (device == total - 3) | (device == total - 2)


def halves(value):
    high = value.astype(jnp.bfloat16)
    low = (value - high.astype(jnp.float32)).astype(jnp.bfloat16)
    return high, low


def dot(left, right):
    return jnp.dot(left, right, preferred_element_type=jnp.float32)


def product(parts, pair):
    width = pair.shape[1] // 2
    odd = len(parts) % 2
    split = [halves(part) for part in parts]
    high = jnp.concatenate([one[0] for one in split] + [split[-1][1]] * odd, 1)
    low = jnp.concatenate([one[1] for one in split[: len(parts) - odd]], 1)
    both = dot(high, pair[...])
    return both[:, :width] + both[:, width:] + dot(low, pair[: low.shape[1], :width])


def neighbours(field, start, rows, stride):
    return [field[pl.ds(start + shift, rows), :] for shift in (0, 1, -1, stride, -stride)]


def far_rows(capacity):
    stride = capacity // 16
    slots = capacity // CHILDREN
    return 2 * stride + DEG * stride // CHILDREN - slots // 2


def columns(row, lanes):
    return jnp.transpose(jnp.broadcast_to(row, (lanes, lanes)))


def scalar_of(numbers, index):
    return numbers[index : index + 1, 0:1][0, 0]


def pack_kernel(count_in, right_in, coef_in, first, second, numbers, count, right_side, coef, turned, arrivals):
    values = right_side.shape[1]
    depth = first.shape[0] - 8
    copies = (
        pltpu.make_async_copy(count_in, count, arrivals.at[0]),
        pltpu.make_async_copy(right_in, right_side, arrivals.at[1]),
        pltpu.make_async_copy(coef_in, coef.at[pl.ds(0, coef_in.shape[0])], arrivals.at[2]),
    )
    for copy in copies:
        copy.start()
    device = device_number()
    total = device_total()
    coef[pl.ds(coef_in.shape[0], 8 - coef_in.shape[0]), :] = jnp.ones(
        (8 - coef_in.shape[0], values), jnp.float32
    )
    turned[...] = jnp.ones(turned.shape, jnp.float32)
    copies[0].wait()
    rows = lax.broadcasted_iota(jnp.int32, numbers.shape, 0)
    table = jnp.zeros(numbers.shape, jnp.int32)
    for offset in range(-NEAR_CELLS, NEAR_CELLS + 1):
        at = device + offset
        size = jnp.where((at >= 0) & (at < total), count[jnp.clip(at, 0, total - 1)], 0)
        table = jnp.where(rows == offset + NEAR_CELLS, size, table)
    numbers[...] = table
    live = count[device]
    is_even = device % 2 == 0
    tail = live - depth
    copies[2].wait()
    for out, start in (
        (first, jnp.where(is_even, tail, 0)),
        (second, jnp.where(is_even, 0, tail)),
    ):
        row = start // values
        lane = start % values
        turned[:8, :] = pltpu.roll(coef[...], (values - lane) % values, 1)
        lanes = lax.broadcasted_iota(jnp.int32, (8, values), 1)
        near = turned[pl.ds(row, 8), :]
        far = turned[pl.ds(row + 1, 8), :]
        out[depth:, :] = jnp.where(lanes < values - lane, near, far)
    copies[1].wait()
    for out, start in (
        (first, jnp.where(is_even, tail, 0)),
        (second, jnp.where(is_even, 0, tail)),
    ):
        out[:depth, :] = right_side[pl.ds(pl.multiple_of(start, 8), depth), :]


def interior_kernel(
    numbers, right_in, coef_in, cell_in, near_in, far_in, prolong_in,
    coupling, restrict, spread, diag, residual, coef, jacobi, *rest,
):
    updates = rest[:DEG]
    coef_rows, cell_matrix, face_near, face_far, prolong, arrivals = rest[DEG:]
    values = cell_in.shape[0]
    capacity = right_in.shape[0]
    stride = capacity // 16
    depth = (residual.shape[0] - capacity) // 2
    right_side = residual.at[pl.ds(depth, capacity)]
    copies = [
        pltpu.make_async_copy(origin, target, arrivals.at[index])
        for index, (origin, target) in enumerate(
            (
                (cell_in, cell_matrix),
                (near_in, face_near),
                (far_in, face_far),
                (coef_in, coef_rows),
                (right_in, right_side),
                (prolong_in, prolong),
            )
        )
    ]
    for copy in copies:
        copy.start()
    spare = pl.ds(depth + capacity, depth)
    for field in (residual, coef, jacobi) + updates:
        field[spare, :] = jnp.zeros((depth, values), jnp.float32)
    for copy in copies[:5]:
        copy.wait()
    near = face_near[...]
    far = face_far[...]
    last = -jnp.transpose(far)
    blocks = (cell_matrix[...], -near, -jnp.transpose(near), -far, last, last)
    for index, block in enumerate(blocks):
        rows = pl.ds(index * values, values)
        high, low = halves(block)
        coupling[rows, :values] = high
        coupling[rows, values:] = low
    row_index = lax.broadcasted_iota(jnp.int32, (values, values), 0)
    lane_index = lax.broadcasted_iota(jnp.int32, (values, values), 1)
    diagonal = jnp.sum(
        jnp.where(row_index == lane_index, cell_matrix[...], 0.0), axis=0, keepdims=True
    )
    diag[...] = jnp.broadcast_to(diagonal, diag.shape)
    keep, gain = STEPS[0]
    for row in range(capacity // values):
        rows = pl.ds(depth + row * values, values)
        column = columns(coef_rows[row : row + 1, :], values)
        source = residual[rows, :]
        scale = 1.0 / (column + diagonal)
        coef[rows, :] = column
        jacobi[rows, :] = scale
        updates[0][rows, :] = gain * (scale * source)
    end = depth + scalar_of(numbers, NEAR_CELLS)
    for index in range(1, DEG + 1):
        start = depth + index * stride
        span = capacity - 2 * index * stride
        rows = pl.ds(start, span)
        before = updates[index - 1]
        old = residual[rows, :]
        fresh = old - (
            coef[rows, :] * before[rows, :] + product(neighbours(before, start, span, stride), coupling)
        )
        inside = start + lax.broadcasted_iota(jnp.int32, (span, values), 0) < end - index * stride
        residual[rows, :] = jnp.where(inside, fresh, old)
        if index < DEG:
            keep, gain = STEPS[index]
            updates[index][rows, :] = keep * before[rows, :] + gain * (jacobi[rows, :] * fresh)
    copies[5].wait()
    for child in range(CHILDREN):
        rows = pl.ds(child * values, values)
        block = prolong[child]
        high, low = halves(block)
        spread[:values, rows] = high
        spread[values:, rows] = low
        high, low = halves(jnp.transpose(block))
        restrict[rows, :values] = high
        restrict[rows, values:] = low


def boundary_kernel(
    numbers, first, second, coupling, restrict, diag, *fields
):
    residual, coef, jacobi = fields[DEG + 3 : DEG + 6]
    updates = fields[DEG + 6 : 2 * DEG + 6]
    message, far_even, far_odd, coarse, coarse_coef = fields[2 * DEG + 6 :]
    frame, values = residual.shape
    depth = first.shape[0] - 8
    capacity = frame - 2 * depth
    stride = capacity // 16
    device = device_number()
    total = device_total()
    is_even = device % 2 == 0
    end = pl.multiple_of(depth + scalar_of(numbers, NEAR_CELLS), 8)
    diagonal = diag[0:1, :]
    left = jnp.where(is_even, second[...], first[...])
    right = jnp.where(is_even, first[...], second[...])
    keep, gain = STEPS[0]
    for side, start, exists in ((left, 0, device > 0), (right, end, device < total - 1)):
        pieces = []
        for row in range(-(-depth // values)):
            pieces.append(columns(side[depth + row : depth + row + 1, :], values))
        column = jnp.concatenate(pieces, 0)[:depth]
        scale = jnp.where(exists, 1.0 / (column + diagonal), 0.0)
        rows = pl.ds(start, depth)
        residual[rows, :] = side[:depth]
        coef[rows, :] = column
        jacobi[rows, :] = scale
        updates[0][rows, :] = gain * (scale * side[:depth])
    for index in range(1, DEG + 1):
        before = updates[index - 1]
        starts = (index * stride, pl.multiple_of(end - index * stride, 8))
        parts = [
            jnp.concatenate([before[pl.ds(start + shift, depth), :] for start in starts], 0)
            for shift in (0, 1, -1, stride, -stride)
        ]
        applied = product(parts, coupling)
        for side, start in enumerate(starts):
            rows = pl.ds(start, depth)
            own = parts[0][side * depth : (side + 1) * depth]
            fresh = residual[rows, :] - (coef[rows, :] * own + applied[side * depth : (side + 1) * depth])
            residual[rows, :] = fresh
            if index < DEG:
                keep, gain = STEPS[index]
                updates[index][rows, :] = keep * own + gain * (jacobi[rows, :] * fresh)
    cells = coarse.shape[0]
    slots = capacity // CHILDREN
    margin = (cells - slots) // 2
    first_row = depth - CHILDREN * margin
    parts = [residual[pl.ds(first_row + c, cells, stride=CHILDREN), :] for c in range(CHILDREN)]
    source = product(parts, restrict)
    coarse[...] = source
    mean = coef[pl.ds(first_row, cells, stride=CHILDREN), :]
    for c in range(1, CHILDREN):
        mean = mean + coef[pl.ds(first_row + c, cells, stride=CHILDREN), :]
    coarse_coef[...] = jnp.zeros(coarse_coef.shape, jnp.float32)
    coarse_coef[:cells, :] = mean * (1.0 / CHILDREN)
    lanes = jnp.transpose(coarse_coef[...])[:8]
    message[:slots, :] = source[margin : margin + slots]
    message[slots:, :] = pltpu.roll(lanes, values - margin, 1)
    count = far_even.shape[0] - 8
    near = far_rows(capacity)
    tail = margin + scalar_of(numbers, NEAR_CELLS) // CHILDREN - near
    is_low = device % 4 < 2
    for out, start in ((far_even, jnp.where(is_low, tail, margin)), (far_odd, jnp.where(is_low, margin, tail))):
        out[:count, :] = coarse[pl.ds(start, count), :]
        out[count:, :] = pltpu.roll(lanes, values - start, 1)


def coarse_kernel(
    numbers, residual, coef, jacobi, *rest
):
    presmoothed = rest[:DEG]
    own, one_a, one_b, one_c, two_a, two_b, coupling, spread, diag, out_hbm = rest[DEG : DEG + 10]
    source, coarse_coef, coarse_jacobi = rest[DEG + 10 : DEG + 13]
    coarse_updates = rest[DEG + 13 : 2 * DEG + 13]
    updates = rest[2 * DEG + 13 : 3 * DEG + 13]
    out, sent = rest[3 * DEG + 13 :]
    capacity, values = out.shape
    stride = capacity // 16
    slots = capacity // CHILDREN
    near = far_rows(capacity)
    margin = 16
    depth = (residual.shape[0] - capacity) // 2
    reach = depth // 2 // CHILDREN
    base = slots + 3 * margin
    device = device_number()
    total = device_total()

    def cells_of(offset):
        return scalar_of(numbers, NEAR_CELLS + offset) // CHILDREN

    start_before = base - cells_of(-1)
    start_after = base + cells_of(0)
    start_last = start_after + cells_of(1)
    source[...] = jnp.zeros(source.shape, jnp.float32)
    coarse_coef[...] = jnp.zeros(coarse_coef.shape, jnp.float32)
    is_even = device % 2 == 0
    is_low = device % 4 < 2
    one_odd = jnp.where(is_near_end(device, total), one_c[...], one_b[...])
    before_one = jnp.where(is_even, one_odd, one_a[...])
    after_one = jnp.where(is_even, one_a[...], one_odd)
    before_two = jnp.where(is_low, two_b[...], two_a[...])
    after_two = jnp.where(is_low, two_a[...], two_b[...])
    placed = (
        (before_two, start_before - near),
        (before_one, start_before),
        (own, base),
        (after_one, start_after),
        (after_two, start_last),
    )
    for piece, at in placed:
        rows = piece.shape[0] - 8
        source[pl.ds(at, rows), :] = piece[:rows, :]
        coarse_coef[pl.ds(at, rows), :] = columns(piece[rows : rows + 1, :], values)[:rows]
    beyond = cells_of(-2) + jnp.where(device > 2, margin, 0)
    lowest = start_before - jnp.minimum(beyond, near)
    beyond = cells_of(2) + jnp.where(device < total - 3, margin, 0)
    highest = start_last + jnp.minimum(beyond, near)
    row_index = lax.broadcasted_iota(jnp.int32, source.shape, 0)
    inside = (row_index >= lowest) & (row_index < highest)
    coarse_jacobi[...] = jnp.where(inside, 1.0 / (coarse_coef[...] + diag[0:1, :]), 0.0)
    coarse_updates[0][...] = STEPS[0][1] * (coarse_jacobi[...] * source[...])
    for index in range(1, DEG):
        keep, gain = STEPS[index]
        before = coarse_updates[index - 1]
        start = base - margin - (DEG - 1 - index) * stride
        span = slots + 2 * margin + 2 * (DEG - 1 - index) * stride
        rows = pl.ds(start, span)
        own_update = before[rows, :]
        fresh = source[rows, :] - (
            coarse_coef[rows, :] * own_update + product(neighbours(before, start, span, stride), coupling)
        )
        source[rows, :] = fresh
        coarse_updates[index][rows, :] = keep * own_update + gain * (coarse_jacobi[rows, :] * fresh)
    count_rows = slots + 2 * reach
    rows = pl.ds(base - reach, count_rows)
    correction = coarse_updates[0][rows, :]
    for index in range(1, DEG):
        correction = correction + coarse_updates[index][rows, :]
    high_part, low_part = halves(correction)
    spread_high = spread[:values, :]
    children = dot(high_part, spread_high) + dot(low_part, spread_high) + dot(high_part, spread[values:, :])
    first_row = depth - CHILDREN * reach
    for c in range(CHILDREN):
        updates[0][pl.ds(first_row + c, count_rows, stride=CHILDREN), :] = children[:, c * values : (c + 1) * values]
    for index in range(DEG):
        keep, gain = STEPS[index]
        before = updates[index]
        begin = first_row + (index + 1) * stride
        span = (CHILDREN * count_rows - 2 * (index + 1) * stride) // 2
        for block in range(2):
            start = begin + block * span
            rows = pl.ds(start, span)
            own_update = before[rows, :]
            fresh = residual[rows, :] - (
                coef[rows, :] * own_update + product(neighbours(before, start, span, stride), coupling)
            )
            step = gain * (jacobi[rows, :] * fresh)
            if index > 0:
                step = step + keep * own_update
            if index < DEG - 1:
                residual[rows, :] = fresh
                updates[index + 1][rows, :] = step
            else:
                total_update = step
                for field in presmoothed + updates:
                    total_update = total_update + field[rows, :]
                slot = start - depth
                is_live = slot + lax.broadcasted_iota(jnp.int32, (span, values), 0) < scalar_of(numbers, NEAR_CELLS)
                out[pl.ds(slot, span), :] = jnp.where(is_live, total_update, 0.0)
                pltpu.make_async_copy(
                    out.at[pl.ds(slot, span)], out_hbm.at[pl.ds(slot, span)], sent.at[block]
                ).start()
    for block in range(2):
        piece = pl.ds(block * (capacity // 2), capacity // 2)
        pltpu.make_async_copy(out.at[piece], out_hbm.at[piece], sent.at[block]).wait()


def exchange(block, distance, phase, complete):
    total = lax.axis_size(AXES)
    pairs = []
    for device in range(total - distance):
        if (device // distance) % 2 == phase:
            pairs += [(device, device + distance), (device + distance, device)]
    if complete:
        busy = {source for source, _ in pairs}
        idle = [device for device in range(total) if device not in busy]
        for one, other in zip(idle[0::2], idle[1::2]):
            pairs += [(one, other), (other, one)]
    return move(block, pairs)


def move(block, pairs):
    return lax.ppermute(block, AXES, pairs)


def shards(right_side, cell_coef, fine_count, cell_matrix, face_near, face_far, prolong):
    capacity, values = right_side.shape
    stride = capacity // 16
    depth = 2 * DEG * stride
    frame = capacity + 2 * depth
    slots = capacity // CHILDREN
    margin = 16
    far = -(-far_rows(capacity) // 8) * 8 + 8
    coef_rows = cell_coef.reshape(capacity // values, values)
    f32 = lambda *shape: jax.ShapeDtypeStruct(shape, jnp.float32)
    bf16 = lambda *shape: jax.ShapeDtypeStruct(shape, jnp.bfloat16)
    buffer = lambda *shape: pltpu.VMEM(shape, jnp.float32)
    vmem = pl.BlockSpec(memory_space=pltpu.VMEM)
    hbm = pl.BlockSpec(memory_space=pltpu.HBM)
    params = pltpu.CompilerParams(vmem_limit_bytes=GRANT)
    off_chip = lambda array: pltpu.with_memory_space_constraint(array, pltpu.HBM)

    first, second, numbers = pl.pallas_call(
        pack_kernel,
        out_shape=(
            f32(depth + 8, values),
            f32(depth + 8, values),
            jax.ShapeDtypeStruct((8, values), jnp.int32),
        ),
        in_specs=[hbm, hbm, hbm],
        out_specs=(vmem, vmem, vmem),
        scratch_shapes=[
            pltpu.SMEM(fine_count.shape, jnp.int32),
            buffer(capacity, values),
            buffer(8, values),
            buffer(24, values),
            pltpu.SemaphoreType.DMA((3,)),
        ],
        name="pack",
        compiler_params=params,
    )(off_chip(fine_count), off_chip(right_side), off_chip(coef_rows))
    second_in = exchange(second, 1, 1, True)
    first_in = exchange(first, 1, 0, False)
    prepared = pl.pallas_call(
        interior_kernel,
        out_shape=(
            bf16(6 * values, 2 * values),
            bf16(CHILDREN * values, 2 * values),
            bf16(2 * values, CHILDREN * values),
            f32(8, values),
        )
        + (f32(frame, values),) * (3 + DEG),
        in_specs=[vmem] + [hbm] * 6,
        out_specs=(vmem,) * (7 + DEG),
        scratch_shapes=[
            buffer(*coef_rows.shape),
            buffer(values, values),
            buffer(values, values),
            buffer(values, values),
            buffer(*prolong.shape),
            pltpu.SemaphoreType.DMA((6,)),
        ],
        name="interior",
        compiler_params=params,
    )(numbers, *(off_chip(each) for each in (right_side, coef_rows, cell_matrix, face_near, face_far, prolong)))
    coupling, restrict, spread, diag = prepared[:4]
    *fields, message, far_even, far_odd = pl.pallas_call(
        boundary_kernel,
        out_shape=(f32(frame, values),) * (3 + DEG)
        + (f32(slots + 8, values), f32(far, values), f32(far, values)),
        in_specs=[vmem] * (9 + DEG),
        out_specs=(vmem,) * (6 + DEG),
        scratch_shapes=[buffer(slots + 2 * margin, values), buffer(values, values)],
        input_output_aliases={6 + index: index for index in range(3 + DEG)},
        name="boundary",
        compiler_params=params,
    )(numbers, first_in, second_in, coupling, restrict, diag, *prepared[4:])
    total = lax.axis_size(AXES)
    ring = [(0, 1), (1, 2), (2, 0), (total - 3, total - 2), (total - 2, total - 1), (total - 1, total - 3)]
    for device in range(3, total - 3, 2):
        ring += [(device, device + 1), (device + 1, device)]
    one_b = move(message, ring)
    ends = [(1, 2), (2, 1), (0, 3), (3, 0)]
    ends += [(total - 1 - source, total - 1 - target) for source, target in ends]
    for device in range(4, total - 4):
        ends += [(device, device + 2 if device % 4 < 2 else device - 2)]
    one_c = move(message, ends)
    two_b = exchange(far_odd, 2, 1, True)
    one_a = exchange(message, 1, 0, False)
    two_a = exchange(far_even, 2, 0, False)
    coarse_frame = 4 * slots + 4 * margin
    return pl.pallas_call(
        coarse_kernel,
        out_shape=f32(capacity, values),
        in_specs=[vmem] * (4 + DEG + 9),
        out_specs=hbm,
        scratch_shapes=[buffer(coarse_frame, values)] * (3 + DEG)
        + [buffer(frame, values)] * DEG
        + [buffer(capacity, values), pltpu.SemaphoreType.DMA((2,))],
        name="coarse",
        compiler_params=params,
    )(numbers, *fields, message, one_a, one_b, one_c, two_a, two_b, coupling, spread, diag)


def solution(mesh):
    placed = (P(AXES, None), P(AXES), P(), P(), P(), P(), P())
    return jax.shard_map(
        shards, mesh=mesh, in_specs=placed, out_specs=P(AXES, None), check_vma=False
    )
```

```python
import jax
import jax.numpy as jnp
from jax import lax
from jax.experimental import pallas as pl
from jax.experimental.pallas import tpu as pltpu
from jax.sharding import PartitionSpec as P

DEG = 3
AXES = ("sfc", "lvl")
CENTER = 1.025
RADIUS = 0.775
CHILDREN = 8
NEAR_CELLS = 2
GRANT = 16 * 1024 * 1024


def chebyshev_weights():
    sigma = CENTER / RADIUS
    weight = 1.0 / sigma
    steps = [(0.0, 1.0 / CENTER)]
    for _ in range(DEG - 1):
        following = 1.0 / (2.0 * sigma - weight)
        steps.append((following * weight, 2.0 * following / RADIUS))
        weight = following
    return steps


STEPS = chebyshev_weights()


def device_number():
    return lax.axis_index("sfc") * lax.axis_size("lvl") + lax.axis_index("lvl")


def device_total():
    return lax.axis_size("sfc") * lax.axis_size("lvl")


def is_near_end(device, total):
    return (device == 2) | (device == total - 3)


def halves(value):
    high = value.astype(jnp.bfloat16)
    low = (value - high.astype(jnp.float32)).astype(jnp.bfloat16)
    return high, low


def dot(left, right):
    return jnp.dot(left, right, preferred_element_type=jnp.float32)


def product(parts, pair):
    width = pair.shape[1] // 2
    odd = len(parts) % 2
    split = [halves(part) for part in parts]
    high = jnp.concatenate([one[0] for one in split] + [split[-1][1]] * odd, 1)
    low = jnp.concatenate([one[1] for one in split[: len(parts) - odd]], 1)
    both = dot(high, pair[...])
    return both[:, :width] + both[:, width:] + dot(low, pair[: low.shape[1], :width])


def neighbours(field, start, rows, stride):
    return [field[pl.ds(start + shift, rows), :] for shift in (0, 1, -1, stride, -stride)]


def far_rows(capacity):
    stride = capacity // 16
    slots = capacity // CHILDREN
    return 2 * stride + DEG * stride // CHILDREN - slots // 2


def columns(row, lanes):
    return jnp.transpose(jnp.broadcast_to(row, (lanes, lanes)))


def scalar_of(numbers, index):
    return numbers[index : index + 1, 0:1][0, 0]


def pack_kernel(count_in, right_in, coef_in, first, second, numbers, count, right_side, coef, turned, arrivals):
    values = right_side.shape[1]
    depth = first.shape[0] - 8
    copies = (
        pltpu.make_async_copy(count_in, count, arrivals.at[0]),
        pltpu.make_async_copy(right_in, right_side, arrivals.at[1]),
        pltpu.make_async_copy(coef_in, coef.at[pl.ds(0, coef_in.shape[0])], arrivals.at[2]),
    )
    for copy in copies:
        copy.start()
    device = device_number()
    total = device_total()
    coef[pl.ds(coef_in.shape[0], 8 - coef_in.shape[0]), :] = jnp.ones(
        (8 - coef_in.shape[0], values), jnp.float32
    )
    turned[...] = jnp.ones(turned.shape, jnp.float32)
    copies[0].wait()
    rows = lax.broadcasted_iota(jnp.int32, numbers.shape, 0)
    table = jnp.zeros(numbers.shape, jnp.int32)
    for offset in range(-NEAR_CELLS, NEAR_CELLS + 1):
        at = device + offset
        size = jnp.where((at >= 0) & (at < total), count[jnp.clip(at, 0, total - 1)], 0)
        table = jnp.where(rows == offset + NEAR_CELLS, size, table)
    numbers[...] = table
    live = count[device]
    is_even = device % 2 == 0
    tail = live - depth
    copies[2].wait()
    for out, start in (
        (first, jnp.where(is_even, tail, 0)),
        (second, jnp.where(is_even, 0, tail)),
    ):
        row = start // values
        lane = start % values
        turned[:8, :] = pltpu.roll(coef[...], (values - lane) % values, 1)
        lanes = lax.broadcasted_iota(jnp.int32, (8, values), 1)
        near = turned[pl.ds(row, 8), :]
        far = turned[pl.ds(row + 1, 8), :]
        out[depth:, :] = jnp.where(lanes < values - lane, near, far)
    copies[1].wait()
    for out, start in (
        (first, jnp.where(is_even, tail, 0)),
        (second, jnp.where(is_even, 0, tail)),
    ):
        out[:depth, :] = right_side[pl.ds(pl.multiple_of(start, 8), depth), :]


def interior_kernel(
    numbers, right_in, coef_in, cell_in, near_in, far_in, prolong_in,
    coupling, restrict, spread, diag, residual, coef, jacobi, *rest,
):
    updates = rest[:DEG]
    coef_rows, cell_matrix, face_near, face_far, prolong, arrivals = rest[DEG:]
    values = cell_in.shape[0]
    capacity = right_in.shape[0]
    stride = capacity // 16
    depth = (residual.shape[0] - capacity) // 2
    right_side = residual.at[pl.ds(depth, capacity)]
    copies = [
        pltpu.make_async_copy(origin, target, arrivals.at[index])
        for index, (origin, target) in enumerate(
            (
                (cell_in, cell_matrix),
                (near_in, face_near),
                (far_in, face_far),
                (coef_in, coef_rows),
                (right_in, right_side),
                (prolong_in, prolong),
            )
        )
    ]
    for copy in copies:
        copy.start()
    spare = pl.ds(depth + capacity, depth)
    for field in (residual, coef, jacobi) + updates:
        field[spare, :] = jnp.zeros((depth, values), jnp.float32)
    for copy in copies[:5]:
        copy.wait()
    near = face_near[...]
    far = face_far[...]
    last = -jnp.transpose(far)
    blocks = (cell_matrix[...], -near, -jnp.transpose(near), -far, last, last)
    for index, block in enumerate(blocks):
        rows = pl.ds(index * values, values)
        high, low = halves(block)
        coupling[rows, :values] = high
        coupling[rows, values:] = low
    row_index = lax.broadcasted_iota(jnp.int32, (values, values), 0)
    lane_index = lax.broadcasted_iota(jnp.int32, (values, values), 1)
    diagonal = jnp.sum(
        jnp.where(row_index == lane_index, cell_matrix[...], 0.0), axis=0, keepdims=True
    )
    diag[...] = jnp.broadcast_to(diagonal, diag.shape)
    keep, gain = STEPS[0]
    for row in range(capacity // values):
        rows = pl.ds(depth + row * values, values)
        column = columns(coef_rows[row : row + 1, :], values)
        source = residual[rows, :]
        scale = 1.0 / (column + diagonal)
        coef[rows, :] = column
        jacobi[rows, :] = scale
        updates[0][rows, :] = gain * (scale * source)
    end = depth + scalar_of(numbers, NEAR_CELLS)
    for index in range(1, DEG + 1):
        start = depth + index * stride
        span = capacity - 2 * index * stride
        rows = pl.ds(start, span)
        before = updates[index - 1]
        old = residual[rows, :]
        fresh = old - (
            coef[rows, :] * before[rows, :] + product(neighbours(before, start, span, stride), coupling)
        )
        inside = start + lax.broadcasted_iota(jnp.int32, (span, values), 0) < end - index * stride
        residual[rows, :] = jnp.where(inside, fresh, old)
        if index < DEG:
            keep, gain = STEPS[index]
            updates[index][rows, :] = keep * before[rows, :] + gain * (jacobi[rows, :] * fresh)
    copies[5].wait()
    for child in range(CHILDREN):
        rows = pl.ds(child * values, values)
        block = prolong[child]
        high, low = halves(block)
        spread[:values, rows] = high
        spread[values:, rows] = low
        high, low = halves(jnp.transpose(block))
        restrict[rows, :values] = high
        restrict[rows, values:] = low


def boundary_kernel(
    numbers, first, second, third, coupling, restrict, diag, *fields
):
    residual, coef, jacobi = fields[DEG + 3 : DEG + 6]
    updates = fields[DEG + 6 : 2 * DEG + 6]
    message, far_even, far_odd, coarse, coarse_coef = fields[2 * DEG + 6 :]
    frame, values = residual.shape
    depth = first.shape[0] - 8
    capacity = frame - 2 * depth
    stride = capacity // 16
    device = device_number()
    total = device_total()
    is_even = device % 2 == 0
    end = pl.multiple_of(depth + scalar_of(numbers, NEAR_CELLS), 8)
    diagonal = diag[0:1, :]
    odd = jnp.where(is_near_end(device, total), third[...], second[...])
    left = jnp.where(is_even, odd, first[...])
    right = jnp.where(is_even, first[...], odd)
    keep, gain = STEPS[0]
    for side, start, exists in ((left, 0, device > 0), (right, end, device < total - 1)):
        pieces = []
        for row in range(-(-depth // values)):
            pieces.append(columns(side[depth + row : depth + row + 1, :], values))
        column = jnp.concatenate(pieces, 0)[:depth]
        scale = jnp.where(exists, 1.0 / (column + diagonal), 0.0)
        rows = pl.ds(start, depth)
        residual[rows, :] = side[:depth]
        coef[rows, :] = column
        jacobi[rows, :] = scale
        updates[0][rows, :] = gain * (scale * side[:depth])
    for index in range(1, DEG + 1):
        before = updates[index - 1]
        starts = (index * stride, pl.multiple_of(end - index * stride, 8))
        parts = [
            jnp.concatenate([before[pl.ds(start + shift, depth), :] for start in starts], 0)
            for shift in (0, 1, -1, stride, -stride)
        ]
        applied = product(parts, coupling)
        for side, start in enumerate(starts):
            rows = pl.ds(start, depth)
            own = parts[0][side * depth : (side + 1) * depth]
            fresh = residual[rows, :] - (coef[rows, :] * own + applied[side * depth : (side + 1) * depth])
            residual[rows, :] = fresh
            if index < DEG:
                keep, gain = STEPS[index]
                updates[index][rows, :] = keep * own + gain * (jacobi[rows, :] * fresh)
    cells = coarse.shape[0]
    slots = capacity // CHILDREN
    margin = (cells - slots) // 2
    first_row = depth - CHILDREN * margin
    parts = [residual[pl.ds(first_row + c, cells, stride=CHILDREN), :] for c in range(CHILDREN)]
    source = product(parts, restrict)
    coarse[...] = source
    mean = coef[pl.ds(first_row, cells, stride=CHILDREN), :]
    for c in range(1, CHILDREN):
        mean = mean + coef[pl.ds(first_row + c, cells, stride=CHILDREN), :]
    coarse_coef[...] = jnp.zeros(coarse_coef.shape, jnp.float32)
    coarse_coef[:cells, :] = mean * (1.0 / CHILDREN)
    lanes = jnp.transpose(coarse_coef[...])[:8]
    message[:slots, :] = source[margin : margin + slots]
    message[slots:, :] = pltpu.roll(lanes, values - margin, 1)
    count = far_even.shape[0] - 8
    near = far_rows(capacity)
    tail = margin + scalar_of(numbers, NEAR_CELLS) // CHILDREN - near
    is_low = device % 4 < 2
    for out, start in ((far_even, jnp.where(is_low, tail, margin)), (far_odd, jnp.where(is_low, margin, tail))):
        out[:count, :] = coarse[pl.ds(start, count), :]
        out[count:, :] = pltpu.roll(lanes, values - start, 1)


def coarse_kernel(
    numbers, residual, coef, jacobi, *rest
):
    presmoothed = rest[:DEG]
    own, one_a, one_b, one_c, two_a, two_b, coupling, spread, diag, out_hbm = rest[DEG : DEG + 10]
    source, coarse_coef, coarse_jacobi = rest[DEG + 10 : DEG + 13]
    coarse_updates = rest[DEG + 13 : 2 * DEG + 13]
    updates = rest[2 * DEG + 13 : 3 * DEG + 13]
    out, sent = rest[3 * DEG + 13 :]
    capacity, values = out.shape
    stride = capacity // 16
    slots = capacity // CHILDREN
    near = far_rows(capacity)
    margin = 16
    depth = (residual.shape[0] - capacity) // 2
    reach = depth // 2 // CHILDREN
    base = slots + 3 * margin
    device = device_number()
    total = device_total()

    def cells_of(offset):
        return scalar_of(numbers, NEAR_CELLS + offset) // CHILDREN

    start_before = base - cells_of(-1)
    start_after = base + cells_of(0)
    start_last = start_after + cells_of(1)
    source[...] = jnp.zeros(source.shape, jnp.float32)
    coarse_coef[...] = jnp.zeros(coarse_coef.shape, jnp.float32)
    is_even = device % 2 == 0
    is_low = device % 4 < 2
    one_odd = jnp.where(is_near_end(device, total), one_c[...], one_b[...])
    before_one = jnp.where(is_even, one_odd, one_a[...])
    after_one = jnp.where(is_even, one_a[...], one_odd)
    before_two = jnp.where(is_low, two_b[...], two_a[...])
    after_two = jnp.where(is_low, two_a[...], two_b[...])
    placed = (
        (before_two, start_before - near),
        (before_one, start_before),
        (own, base),
        (after_one, start_after),
        (after_two, start_last),
    )
    for piece, at in placed:
        rows = piece.shape[0] - 8
        source[pl.ds(at, rows), :] = piece[:rows, :]
        coarse_coef[pl.ds(at, rows), :] = columns(piece[rows : rows + 1, :], values)[:rows]
    beyond = cells_of(-2) + jnp.where(device > 2, margin, 0)
    lowest = start_before - jnp.minimum(beyond, near)
    beyond = cells_of(2) + jnp.where(device < total - 3, margin, 0)
    highest = start_last + jnp.minimum(beyond, near)
    row_index = lax.broadcasted_iota(jnp.int32, source.shape, 0)
    inside = (row_index >= lowest) & (row_index < highest)
    coarse_jacobi[...] = jnp.where(inside, 1.0 / (coarse_coef[...] + diag[0:1, :]), 0.0)
    coarse_updates[0][...] = STEPS[0][1] * (coarse_jacobi[...] * source[...])
    for index in range(1, DEG):
        keep, gain = STEPS[index]
        before = coarse_updates[index - 1]
        start = base - margin - (DEG - 1 - index) * stride
        span = slots + 2 * margin + 2 * (DEG - 1 - index) * stride
        rows = pl.ds(start, span)
        own_update = before[rows, :]
        fresh = source[rows, :] - (
            coarse_coef[rows, :] * own_update + product(neighbours(before, start, span, stride), coupling)
        )
        source[rows, :] = fresh
        coarse_updates[index][rows, :] = keep * own_update + gain * (coarse_jacobi[rows, :] * fresh)
    count_rows = slots + 2 * reach
    rows = pl.ds(base - reach, count_rows)
    correction = coarse_updates[0][rows, :]
    for index in range(1, DEG):
        correction = correction + coarse_updates[index][rows, :]
    high_part, low_part = halves(correction)
    spread_high = spread[:values, :]
    children = dot(high_part, spread_high) + dot(low_part, spread_high) + dot(high_part, spread[values:, :])
    first_row = depth - CHILDREN * reach
    for c in range(CHILDREN):
        updates[0][pl.ds(first_row + c, count_rows, stride=CHILDREN), :] = children[:, c * values : (c + 1) * values]
    for index in range(DEG):
        keep, gain = STEPS[index]
        before = updates[index]
        begin = first_row + (index + 1) * stride
        span = (CHILDREN * count_rows - 2 * (index + 1) * stride) // 2
        for block in range(2):
            start = begin + block * span
            rows = pl.ds(start, span)
            own_update = before[rows, :]
            fresh = residual[rows, :] - (
                coef[rows, :] * own_update + product(neighbours(before, start, span, stride), coupling)
            )
            step = gain * (jacobi[rows, :] * fresh)
            if index > 0:
                step = step + keep * own_update
            if index < DEG - 1:
                residual[rows, :] = fresh
                updates[index + 1][rows, :] = step
            else:
                total_update = step
                for field in presmoothed + updates:
                    total_update = total_update + field[rows, :]
                slot = start - depth
                is_live = slot + lax.broadcasted_iota(jnp.int32, (span, values), 0) < scalar_of(numbers, NEAR_CELLS)
                out[pl.ds(slot, span), :] = jnp.where(is_live, total_update, 0.0)
                pltpu.make_async_copy(
                    out.at[pl.ds(slot, span)], out_hbm.at[pl.ds(slot, span)], sent.at[block]
                ).start()
    for block in range(2):
        piece = pl.ds(block * (capacity // 2), capacity // 2)
        pltpu.make_async_copy(out.at[piece], out_hbm.at[piece], sent.at[block]).wait()


def exchange(block, distance, phase, complete):
    total = lax.axis_size(AXES)
    pairs = []
    for device in range(total - distance):
        if (device // distance) % 2 == phase:
            pairs += [(device, device + distance), (device + distance, device)]
    if complete:
        busy = {source for source, _ in pairs}
        idle = [device for device in range(total) if device not in busy]
        for one, other in zip(idle[0::2], idle[1::2]):
            pairs += [(one, other), (other, one)]
    return move(block, pairs)


def move(block, pairs):
    return lax.ppermute(block, AXES, pairs)


def shards(right_side, cell_coef, fine_count, cell_matrix, face_near, face_far, prolong):
    capacity, values = right_side.shape
    stride = capacity // 16
    depth = 2 * DEG * stride
    frame = capacity + 2 * depth
    slots = capacity // CHILDREN
    margin = 16
    far = -(-far_rows(capacity) // 8) * 8 + 8
    coef_rows = cell_coef.reshape(capacity // values, values)
    f32 = lambda *shape: jax.ShapeDtypeStruct(shape, jnp.float32)
    bf16 = lambda *shape: jax.ShapeDtypeStruct(shape, jnp.bfloat16)
    buffer = lambda *shape: pltpu.VMEM(shape, jnp.float32)
    vmem = pl.BlockSpec(memory_space=pltpu.VMEM)
    hbm = pl.BlockSpec(memory_space=pltpu.HBM)
    params = pltpu.CompilerParams(vmem_limit_bytes=GRANT)
    off_chip = lambda array: pltpu.with_memory_space_constraint(array, pltpu.HBM)

    first, second, numbers = pl.pallas_call(
        pack_kernel,
        out_shape=(
            f32(depth + 8, values),
            f32(depth + 8, values),
            jax.ShapeDtypeStruct((8, values), jnp.int32),
        ),
        in_specs=[hbm, hbm, hbm],
        out_specs=(vmem, vmem, vmem),
        scratch_shapes=[
            pltpu.SMEM(fine_count.shape, jnp.int32),
            buffer(capacity, values),
            buffer(8, values),
            buffer(24, values),
            pltpu.SemaphoreType.DMA((3,)),
        ],
        name="pack",
        compiler_params=params,
    )(off_chip(fine_count), off_chip(right_side), off_chip(coef_rows))
    total = lax.axis_size(AXES)
    ring = [(0, 2), (2, 1), (1, 0)]
    ring += [(total - 1 - source, total - 1 - target) for source, target in ring]
    for device in range(3, total - 3, 2):
        ring += [(device, device + 1), (device + 1, device)]
    ends = [(1, 2), (2, 0), (0, 3), (3, 1)]
    ends += [(total - 1 - source, total - 1 - target) for source, target in ends]
    for device in range(4, total - 4):
        ends += [(device, device + 2 if device % 4 < 2 else device - 2)]
    second_in = move(second, ring)
    third_in = move(second, ends)
    first_in = exchange(first, 1, 0, False)
    prepared = pl.pallas_call(
        interior_kernel,
        out_shape=(
            bf16(6 * values, 2 * values),
            bf16(CHILDREN * values, 2 * values),
            bf16(2 * values, CHILDREN * values),
            f32(8, values),
        )
        + (f32(frame, values),) * (3 + DEG),
        in_specs=[vmem] + [hbm] * 6,
        out_specs=(vmem,) * (7 + DEG),
        scratch_shapes=[
            buffer(*coef_rows.shape),
            buffer(values, values),
            buffer(values, values),
            buffer(values, values),
            buffer(*prolong.shape),
            pltpu.SemaphoreType.DMA((6,)),
        ],
        name="interior",
        compiler_params=params,
    )(numbers, *(off_chip(each) for each in (right_side, coef_rows, cell_matrix, face_near, face_far, prolong)))
    coupling, restrict, spread, diag = prepared[:4]
    *fields, message, far_even, far_odd = pl.pallas_call(
        boundary_kernel,
        out_shape=(f32(frame, values),) * (3 + DEG)
        + (f32(slots + 8, values), f32(far, values), f32(far, values)),
        in_specs=[vmem] * (10 + DEG),
        out_specs=(vmem,) * (6 + DEG),
        scratch_shapes=[buffer(slots + 2 * margin, values), buffer(values, values)],
        input_output_aliases={7 + index: index for index in range(3 + DEG)},
        name="boundary",
        compiler_params=params,
    )(numbers, first_in, second_in, third_in, coupling, restrict, diag, *prepared[4:])
    one_b = move(message, ring)
    one_c = move(message, ends)
    two_b = exchange(far_odd, 2, 1, True)
    one_a = exchange(message, 1, 0, False)
    two_a = exchange(far_even, 2, 0, False)
    coarse_frame = 4 * slots + 4 * margin
    return pl.pallas_call(
        coarse_kernel,
        out_shape=f32(capacity, values),
        in_specs=[vmem] * (4 + DEG + 9),
        out_specs=hbm,
        scratch_shapes=[buffer(coarse_frame, values)] * (3 + DEG)
        + [buffer(frame, values)] * DEG
        + [buffer(capacity, values), pltpu.SemaphoreType.DMA((2,))],
        name="coarse",
        compiler_params=params,
    )(numbers, *fields, message, one_a, one_b, one_c, two_a, two_b, coupling, spread, diag)


def solution(mesh):
    placed = (P(AXES, None), P(AXES), P(), P(), P(), P(), P())
    return jax.shard_map(
        shards, mesh=mesh, in_specs=placed, out_specs=P(AXES, None), check_vma=False
    )
```

```python
import jax
import jax.numpy as jnp
from jax import lax
from jax.experimental import pallas as pl
from jax.experimental.pallas import tpu as pltpu
from jax.sharding import PartitionSpec as P

DEG = 3
AXES = ("sfc", "lvl")
CENTER = 1.025
RADIUS = 0.775
CHILDREN = 8
NEAR_CELLS = 2
GRANT = 16 * 1024 * 1024


def chebyshev_weights():
    sigma = CENTER / RADIUS
    weight = 1.0 / sigma
    steps = [(0.0, 1.0 / CENTER)]
    for _ in range(DEG - 1):
        following = 1.0 / (2.0 * sigma - weight)
        steps.append((following * weight, 2.0 * following / RADIUS))
        weight = following
    return steps


STEPS = chebyshev_weights()


def device_number():
    return lax.axis_index("sfc") * lax.axis_size("lvl") + lax.axis_index("lvl")


def device_total():
    return lax.axis_size("sfc") * lax.axis_size("lvl")


def is_near_end(device, total):
    return (device == 2) | (device == total - 3)


def halves(value):
    high = value.astype(jnp.bfloat16)
    low = (value - high.astype(jnp.float32)).astype(jnp.bfloat16)
    return high, low


def dot(left, right):
    return jnp.dot(left, right, preferred_element_type=jnp.float32)


def product(parts, pair):
    width = pair.shape[1] // 2
    odd = len(parts) % 2
    split = [halves(part) for part in parts]
    high = jnp.concatenate([one[0] for one in split] + [split[-1][1]] * odd, 1)
    low = jnp.concatenate([one[1] for one in split[: len(parts) - odd]], 1)
    both = dot(high, pair[...])
    return both[:, :width] + both[:, width:] + dot(low, pair[: low.shape[1], :width])


def neighbours(field, start, rows, stride):
    return [field[pl.ds(start + shift, rows), :] for shift in (0, 1, -1, stride, -stride)]


def far_rows(capacity):
    stride = capacity // 16
    slots = capacity // CHILDREN
    return 2 * stride + DEG * stride // CHILDREN - slots // 2


def columns(row, lanes):
    return jnp.transpose(jnp.broadcast_to(row, (lanes, lanes)))


def scalar_of(numbers, index):
    return numbers[index : index + 1, 0:1][0, 0]


def pack_kernel(count_in, right_in, coef_in, first, second, numbers, count, right_side, coef, turned, arrivals):
    values = right_side.shape[1]
    depth = first.shape[0] - 8
    copies = (
        pltpu.make_async_copy(count_in, count, arrivals.at[0]),
        pltpu.make_async_copy(right_in, right_side, arrivals.at[1]),
        pltpu.make_async_copy(coef_in, coef.at[pl.ds(0, coef_in.shape[0])], arrivals.at[2]),
    )
    for copy in copies:
        copy.start()
    device = device_number()
    total = device_total()
    coef[pl.ds(coef_in.shape[0], 8 - coef_in.shape[0]), :] = jnp.ones(
        (8 - coef_in.shape[0], values), jnp.float32
    )
    turned[...] = jnp.ones(turned.shape, jnp.float32)
    copies[0].wait()
    rows = lax.broadcasted_iota(jnp.int32, numbers.shape, 0)
    table = jnp.zeros(numbers.shape, jnp.int32)
    for offset in range(-NEAR_CELLS, NEAR_CELLS + 1):
        at = device + offset
        size = jnp.where((at >= 0) & (at < total), count[jnp.clip(at, 0, total - 1)], 0)
        table = jnp.where(rows == offset + NEAR_CELLS, size, table)
    numbers[...] = table
    live = count[device]
    is_even = device % 2 == 0
    tail = live - depth
    copies[2].wait()
    for out, start in (
        (first, jnp.where(is_even, tail, 0)),
        (second, jnp.where(is_even, 0, tail)),
    ):
        row = start // values
        lane = start % values
        turned[:8, :] = pltpu.roll(coef[...], (values - lane) % values, 1)
        lanes = lax.broadcasted_iota(jnp.int32, (8, values), 1)
        near = turned[pl.ds(row, 8), :]
        far = turned[pl.ds(row + 1, 8), :]
        out[depth:, :] = jnp.where(lanes < values - lane, near, far)
    copies[1].wait()
    for out, start in (
        (first, jnp.where(is_even, tail, 0)),
        (second, jnp.where(is_even, 0, tail)),
    ):
        out[:depth, :] = right_side[pl.ds(pl.multiple_of(start, 8), depth), :]


def interior_kernel(
    numbers, right_in, coef_in, cell_in, near_in, far_in, prolong_in,
    coupling, restrict, diag, residual, coef, jacobi, *rest,
):
    updates = rest[:DEG]
    coef_rows, cell_matrix, face_near, face_far, prolong, arrivals = rest[DEG:]
    values = cell_in.shape[0]
    capacity = right_in.shape[0]
    stride = capacity // 16
    depth = (residual.shape[0] - capacity) // 2
    right_side = residual.at[pl.ds(depth, capacity)]
    copies = [
        pltpu.make_async_copy(origin, target, arrivals.at[index])
        for index, (origin, target) in enumerate(
            (
                (cell_in, cell_matrix),
                (near_in, face_near),
                (far_in, face_far),
                (coef_in, coef_rows),
                (right_in, right_side),
                (prolong_in, prolong),
            )
        )
    ]
    for copy in copies:
        copy.start()
    spare = pl.ds(depth + capacity, depth)
    for field in (residual, coef, jacobi) + updates:
        field[spare, :] = jnp.zeros((depth, values), jnp.float32)
    for copy in copies[:5]:
        copy.wait()
    near = face_near[...]
    far = face_far[...]
    last = -jnp.transpose(far)
    blocks = (cell_matrix[...], -near, -jnp.transpose(near), -far, last, last)
    for index, block in enumerate(blocks):
        rows = pl.ds(index * values, values)
        high, low = halves(block)
        coupling[rows, :values] = high
        coupling[rows, values:] = low
    row_index = lax.broadcasted_iota(jnp.int32, (values, values), 0)
    lane_index = lax.broadcasted_iota(jnp.int32, (values, values), 1)
    diagonal = jnp.sum(
        jnp.where(row_index == lane_index, cell_matrix[...], 0.0), axis=0, keepdims=True
    )
    diag[...] = jnp.broadcast_to(diagonal, diag.shape)
    keep, gain = STEPS[0]
    for row in range(capacity // values):
        rows = pl.ds(depth + row * values, values)
        column = columns(coef_rows[row : row + 1, :], values)
        source = residual[rows, :]
        scale = 1.0 / (column + diagonal)
        coef[rows, :] = column
        jacobi[rows, :] = scale
        updates[0][rows, :] = gain * (scale * source)
    end = depth + scalar_of(numbers, NEAR_CELLS)
    for index in range(1, DEG + 1):
        start = depth + index * stride
        span = capacity - 2 * index * stride
        rows = pl.ds(start, span)
        before = updates[index - 1]
        old = residual[rows, :]
        fresh = old - (
            coef[rows, :] * before[rows, :] + product(neighbours(before, start, span, stride), coupling)
        )
        inside = start + lax.broadcasted_iota(jnp.int32, (span, values), 0) < end - index * stride
        residual[rows, :] = jnp.where(inside, fresh, old)
        if index < DEG:
            keep, gain = STEPS[index]
            updates[index][rows, :] = keep * before[rows, :] + gain * (jacobi[rows, :] * fresh)
    copies[5].wait()
    for child in range(CHILDREN):
        rows = pl.ds(child * values, values)
        block = prolong[child]
        high, low = halves(jnp.transpose(block))
        restrict[rows, :values] = high
        restrict[rows, values:] = low


def spread_kernel(prolong, spread):
    values = prolong.shape[1]
    for child in range(CHILDREN):
        columns_of = pl.ds(child * values, values)
        high, low = halves(prolong[child])
        spread[:values, columns_of] = high
        spread[values:, columns_of] = low


def boundary_kernel(
    numbers, first, second, third, coupling, restrict, diag, *fields
):
    residual, coef, jacobi = fields[DEG + 3 : DEG + 6]
    updates = fields[DEG + 6 : 2 * DEG + 6]
    message, far_even, far_odd, coarse, coarse_coef = fields[2 * DEG + 6 :]
    frame, values = residual.shape
    depth = first.shape[0] - 8
    capacity = frame - 2 * depth
    stride = capacity // 16
    device = device_number()
    total = device_total()
    is_even = device % 2 == 0
    end = pl.multiple_of(depth + scalar_of(numbers, NEAR_CELLS), 8)
    diagonal = diag[0:1, :]
    odd = jnp.where(is_near_end(device, total), third[...], second[...])
    left = jnp.where(is_even, odd, first[...])
    right = jnp.where(is_even, first[...], odd)
    keep, gain = STEPS[0]
    for side, start, exists in ((left, 0, device > 0), (right, end, device < total - 1)):
        pieces = []
        for row in range(-(-depth // values)):
            pieces.append(columns(side[depth + row : depth + row + 1, :], values))
        column = jnp.concatenate(pieces, 0)[:depth]
        scale = jnp.where(exists, 1.0 / (column + diagonal), 0.0)
        rows = pl.ds(start, depth)
        residual[rows, :] = side[:depth]
        coef[rows, :] = column
        jacobi[rows, :] = scale
        updates[0][rows, :] = gain * (scale * side[:depth])
    for index in range(1, DEG + 1):
        before = updates[index - 1]
        starts = (index * stride, pl.multiple_of(end - index * stride, 8))
        parts = [
            jnp.concatenate([before[pl.ds(start + shift, depth), :] for start in starts], 0)
            for shift in (0, 1, -1, stride, -stride)
        ]
        applied = product(parts, coupling)
        for side, start in enumerate(starts):
            rows = pl.ds(start, depth)
            own = parts[0][side * depth : (side + 1) * depth]
            fresh = residual[rows, :] - (coef[rows, :] * own + applied[side * depth : (side + 1) * depth])
            residual[rows, :] = fresh
            if index < DEG:
                keep, gain = STEPS[index]
                updates[index][rows, :] = keep * own + gain * (jacobi[rows, :] * fresh)
    cells = coarse.shape[0]
    slots = capacity // CHILDREN
    margin = (cells - slots) // 2
    first_row = depth - CHILDREN * margin
    parts = [residual[pl.ds(first_row + c, cells, stride=CHILDREN), :] for c in range(CHILDREN)]
    source = product(parts, restrict)
    coarse[...] = source
    mean = coef[pl.ds(first_row, cells, stride=CHILDREN), :]
    for c in range(1, CHILDREN):
        mean = mean + coef[pl.ds(first_row + c, cells, stride=CHILDREN), :]
    coarse_coef[...] = jnp.zeros(coarse_coef.shape, jnp.float32)
    coarse_coef[:cells, :] = mean * (1.0 / CHILDREN)
    lanes = jnp.transpose(coarse_coef[...])[:8]
    message[:slots, :] = source[margin : margin + slots]
    message[slots:, :] = pltpu.roll(lanes, values - margin, 1)
    count = far_even.shape[0] - 8
    near = far_rows(capacity)
    tail = margin + scalar_of(numbers, NEAR_CELLS) // CHILDREN - near
    is_low = device % 4 < 2
    for out, start in ((far_even, jnp.where(is_low, tail, margin)), (far_odd, jnp.where(is_low, margin, tail))):
        out[:count, :] = coarse[pl.ds(start, count), :]
        out[count:, :] = pltpu.roll(lanes, values - start, 1)


def coarse_kernel(
    numbers, residual, coef, jacobi, *rest
):
    presmoothed = rest[:DEG]
    own, one_a, one_b, one_c, two_a, two_b, coupling, spread, diag, out_hbm = rest[DEG : DEG + 10]
    source, coarse_coef, coarse_jacobi = rest[DEG + 10 : DEG + 13]
    coarse_updates = rest[DEG + 13 : 2 * DEG + 13]
    updates = rest[2 * DEG + 13 : 3 * DEG + 13]
    out, sent = rest[3 * DEG + 13 :]
    capacity, values = out.shape
    stride = capacity // 16
    slots = capacity // CHILDREN
    near = far_rows(capacity)
    margin = 16
    depth = (residual.shape[0] - capacity) // 2
    reach = depth // 2 // CHILDREN
    base = slots + 3 * margin
    device = device_number()
    total = device_total()

    def cells_of(offset):
        return scalar_of(numbers, NEAR_CELLS + offset) // CHILDREN

    start_before = base - cells_of(-1)
    start_after = base + cells_of(0)
    start_last = start_after + cells_of(1)
    source[...] = jnp.zeros(source.shape, jnp.float32)
    coarse_coef[...] = jnp.zeros(coarse_coef.shape, jnp.float32)
    is_even = device % 2 == 0
    is_low = device % 4 < 2
    one_odd = jnp.where(is_near_end(device, total), one_c[...], one_b[...])
    before_one = jnp.where(is_even, one_odd, one_a[...])
    after_one = jnp.where(is_even, one_a[...], one_odd)
    before_two = jnp.where(is_low, two_b[...], two_a[...])
    after_two = jnp.where(is_low, two_a[...], two_b[...])
    placed = (
        (before_two, start_before - near),
        (before_one, start_before),
        (own, base),
        (after_one, start_after),
        (after_two, start_last),
    )
    for piece, at in placed:
        rows = piece.shape[0] - 8
        source[pl.ds(at, rows), :] = piece[:rows, :]
        coarse_coef[pl.ds(at, rows), :] = columns(piece[rows : rows + 1, :], values)[:rows]
    beyond = cells_of(-2) + jnp.where(device > 2, margin, 0)
    lowest = start_before - jnp.minimum(beyond, near)
    beyond = cells_of(2) + jnp.where(device < total - 3, margin, 0)
    highest = start_last + jnp.minimum(beyond, near)
    row_index = lax.broadcasted_iota(jnp.int32, source.shape, 0)
    inside = (row_index >= lowest) & (row_index < highest)
    coarse_jacobi[...] = jnp.where(inside, 1.0 / (coarse_coef[...] + diag[0:1, :]), 0.0)
    coarse_updates[0][...] = STEPS[0][1] * (coarse_jacobi[...] * source[...])
    for index in range(1, DEG):
        keep, gain = STEPS[index]
        before = coarse_updates[index - 1]
        start = base - margin - (DEG - 1 - index) * stride
        span = slots + 2 * margin + 2 * (DEG - 1 - index) * stride
        rows = pl.ds(start, span)
        own_update = before[rows, :]
        fresh = source[rows, :] - (
            coarse_coef[rows, :] * own_update + product(neighbours(before, start, span, stride), coupling)
        )
        source[rows, :] = fresh
        coarse_updates[index][rows, :] = keep * own_update + gain * (coarse_jacobi[rows, :] * fresh)
    count_rows = slots + 2 * reach
    rows = pl.ds(base - reach, count_rows)
    correction = coarse_updates[0][rows, :]
    for index in range(1, DEG):
        correction = correction + coarse_updates[index][rows, :]
    high_part, low_part = halves(correction)
    spread_high = spread[:values, :]
    children = dot(high_part, spread_high) + dot(low_part, spread_high) + dot(high_part, spread[values:, :])
    first_row = depth - CHILDREN * reach
    for c in range(CHILDREN):
        updates[0][pl.ds(first_row + c, count_rows, stride=CHILDREN), :] = children[:, c * values : (c + 1) * values]
    for index in range(DEG):
        keep, gain = STEPS[index]
        before = updates[index]
        begin = first_row + (index + 1) * stride
        span = (CHILDREN * count_rows - 2 * (index + 1) * stride) // 2
        for block in range(2):
            start = begin + block * span
            rows = pl.ds(start, span)
            own_update = before[rows, :]
            fresh = residual[rows, :] - (
                coef[rows, :] * own_update + product(neighbours(before, start, span, stride), coupling)
            )
            step = gain * (jacobi[rows, :] * fresh)
            if index > 0:
                step = step + keep * own_update
            if index < DEG - 1:
                residual[rows, :] = fresh
                updates[index + 1][rows, :] = step
            else:
                total_update = step
                for field in presmoothed + updates:
                    total_update = total_update + field[rows, :]
                slot = start - depth
                is_live = slot + lax.broadcasted_iota(jnp.int32, (span, values), 0) < scalar_of(numbers, NEAR_CELLS)
                out[pl.ds(slot, span), :] = jnp.where(is_live, total_update, 0.0)
                pltpu.make_async_copy(
                    out.at[pl.ds(slot, span)], out_hbm.at[pl.ds(slot, span)], sent.at[block]
                ).start()
    for block in range(2):
        piece = pl.ds(block * (capacity // 2), capacity // 2)
        pltpu.make_async_copy(out.at[piece], out_hbm.at[piece], sent.at[block]).wait()


def exchange(block, distance, phase, complete):
    total = lax.axis_size(AXES)
    pairs = []
    for device in range(total - distance):
        if (device // distance) % 2 == phase:
            pairs += [(device, device + distance), (device + distance, device)]
    if complete:
        busy = {source for source, _ in pairs}
        idle = [device for device in range(total) if device not in busy]
        for one, other in zip(idle[0::2], idle[1::2]):
            pairs += [(one, other), (other, one)]
    return move(block, pairs)


def move(block, pairs):
    return lax.ppermute(block, AXES, pairs)


def shards(right_side, cell_coef, fine_count, cell_matrix, face_near, face_far, prolong):
    capacity, values = right_side.shape
    stride = capacity // 16
    depth = 2 * DEG * stride
    frame = capacity + 2 * depth
    slots = capacity // CHILDREN
    margin = 16
    far = -(-far_rows(capacity) // 8) * 8 + 8
    coef_rows = cell_coef.reshape(capacity // values, values)
    f32 = lambda *shape: jax.ShapeDtypeStruct(shape, jnp.float32)
    bf16 = lambda *shape: jax.ShapeDtypeStruct(shape, jnp.bfloat16)
    buffer = lambda *shape: pltpu.VMEM(shape, jnp.float32)
    vmem = pl.BlockSpec(memory_space=pltpu.VMEM)
    hbm = pl.BlockSpec(memory_space=pltpu.HBM)
    params = pltpu.CompilerParams(vmem_limit_bytes=GRANT)
    off_chip = lambda array: pltpu.with_memory_space_constraint(array, pltpu.HBM)

    first, second, numbers = pl.pallas_call(
        pack_kernel,
        out_shape=(
            f32(depth + 8, values),
            f32(depth + 8, values),
            jax.ShapeDtypeStruct((8, values), jnp.int32),
        ),
        in_specs=[hbm, hbm, hbm],
        out_specs=(vmem, vmem, vmem),
        scratch_shapes=[
            pltpu.SMEM(fine_count.shape, jnp.int32),
            buffer(capacity, values),
            buffer(8, values),
            buffer(24, values),
            pltpu.SemaphoreType.DMA((3,)),
        ],
        name="pack",
        compiler_params=params,
    )(off_chip(fine_count), off_chip(right_side), off_chip(coef_rows))
    total = lax.axis_size(AXES)
    ring = [(0, 2), (2, 1), (1, 0)]
    ring += [(total - 1 - source, total - 1 - target) for source, target in ring]
    for device in range(3, total - 3, 2):
        ring += [(device, device + 1), (device + 1, device)]
    ends = [(1, 2), (2, 0), (0, 3), (3, 1)]
    ends += [(total - 1 - source, total - 1 - target) for source, target in ends]
    for device in range(4, total - 4):
        ends += [(device, device + 2 if device % 4 < 2 else device - 2)]
    second_in = move(second, ring)
    third_in = move(second, ends)
    first_in = exchange(first, 1, 0, False)
    prepared = pl.pallas_call(
        interior_kernel,
        out_shape=(
            bf16(6 * values, 2 * values),
            bf16(CHILDREN * values, 2 * values),
            f32(8, values),
        )
        + (f32(frame, values),) * (3 + DEG),
        in_specs=[vmem] + [hbm] * 6,
        out_specs=(vmem,) * (6 + DEG),
        scratch_shapes=[
            buffer(*coef_rows.shape),
            buffer(values, values),
            buffer(values, values),
            buffer(values, values),
            buffer(*prolong.shape),
            pltpu.SemaphoreType.DMA((6,)),
        ],
        name="interior",
        compiler_params=params,
    )(numbers, *(off_chip(each) for each in (right_side, coef_rows, cell_matrix, face_near, face_far, prolong)))
    coupling, restrict, diag = prepared[:3]
    *fields, message, far_even, far_odd = pl.pallas_call(
        boundary_kernel,
        out_shape=(f32(frame, values),) * (3 + DEG)
        + (f32(slots + 8, values), f32(far, values), f32(far, values)),
        in_specs=[vmem] * (10 + DEG),
        out_specs=(vmem,) * (6 + DEG),
        scratch_shapes=[buffer(slots + 2 * margin, values), buffer(values, values)],
        input_output_aliases={7 + index: index for index in range(3 + DEG)},
        name="boundary",
        compiler_params=params,
    )(numbers, first_in, second_in, third_in, coupling, restrict, diag, *prepared[3:])
    one_b = move(message, ring)
    one_c = move(message, ends)
    two_b = exchange(far_odd, 2, 1, True)
    one_a = exchange(message, 1, 0, False)
    two_a = exchange(far_even, 2, 0, False)
    spread = pl.pallas_call(
        spread_kernel,
        out_shape=bf16(2 * values, CHILDREN * values),
        in_specs=[vmem],
        out_specs=vmem,
        name="spread",
        compiler_params=params,
    )(prolong)
    coarse_frame = 4 * slots + 4 * margin
    return pl.pallas_call(
        coarse_kernel,
        out_shape=f32(capacity, values),
        in_specs=[vmem] * (4 + DEG + 9),
        out_specs=hbm,
        scratch_shapes=[buffer(coarse_frame, values)] * (3 + DEG)
        + [buffer(frame, values)] * DEG
        + [buffer(capacity, values), pltpu.SemaphoreType.DMA((2,))],
        name="coarse",
        compiler_params=params,
    )(numbers, *fields, message, one_a, one_b, one_c, two_a, two_b, coupling, spread, diag)


def solution(mesh):
    placed = (P(AXES, None), P(AXES), P(), P(), P(), P(), P())
    return jax.shard_map(
        shards, mesh=mesh, in_specs=placed, out_specs=P(AXES, None), check_vma=False
    )
```
